256 devices in a mesh: space: 128 (over y, z, x), grp: 2 (over core).
Axes of the slice: x: 4, y: 4, z: 8, core: 2. Of those that a mesh axis runs over, the one named last changes fastest.
Arguments:
- echoes: bfloat16 [1280, 300, 2048], P(('space', 'grp'))
- frame_count: int32 [1280], replicated, may hold values from 0 to 300, as said below
- clutter_rank: int32 [1280], replicated, may hold values from 1 to 24
- noise_rank: int32 [1280], replicated, may hold values from 48 to 96
- start_basis: float32 [300, 96], replicated, may hold values from -6 to 6
Outputs:
- volume: float32 [300, 1310720], P(None, ('space', 'grp'))
- power: float32 [1310720], P(('space', 'grp'))
The draws below stay inside these ranges and needn't reach their ends.
Inputs may be any that keep to these rules, and one draw needn't show every extreme that they name: `frame_count`: within each holder's 5 consecutive slots the slots with frames come first and the others have 0 frames; every holder has 1 to 5 slots with frames, some holder has all 5; two holders with the same grp index whose space indices lie half the space axis apart have at most 6 slots with frames together; a slot with frames has 150 or more.
All inputs are finite; a program needn't handle non-finite values.
Results may differ from the reference program's by a relative error of at most 0.0056.
Values may be sent and summed in bfloat16 or wider, within the bound.
A program may use at most 128 MiB of HBM per device.

```python
import jax
import jax.numpy as jnp
from jax import lax

F = 300
V = 2048
K = 96
ITERS = 4
HOLD = 5
OWN = 3
BLOCKS = 1280
N_SPACE = 128
N_GRP = 2


def live_counts(key):
    half_space = N_SPACE // 2
    first_key, second_key, third_key = jax.random.split(jax.random.fold_in(key, 7), 3)
    totals = jax.random.randint(first_key, (half_space, N_GRP), OWN + 2, 2 * OWN + 1)
    rows = jnp.arange(half_space)[:, None]
    cols = jnp.arange(N_GRP)[None, :]
    corner = (rows == 0) & (cols == 0)
    last_pair = (rows == half_space - 1) & (cols == N_GRP - 1)
    totals = jnp.where(corner, 2 * OWN, totals)
    lowest = OWN + 1
    highest = jnp.minimum(HOLD, totals - 1)
    random_bits = jax.random.randint(second_key, (half_space, N_GRP), 0, 1 << 20)
    larger = lowest + random_bits % (highest - lowest + 1)
    larger = jnp.where(corner, HOLD, larger)
    smaller = totals - larger
    flip_bits = jax.random.randint(third_key, (half_space, N_GRP), 0, 2)
    flip_bits = jnp.where(corner | last_pair, 0, flip_bits)
    first_counts = jnp.where(flip_bits == 0, larger, smaller)
    second_counts = jnp.where(flip_bits == 0, smaller, larger)
    return jnp.concatenate([first_counts, second_counts], axis=0).reshape(-1)


def draw_frame_count(key, part):
    counts = live_counts(key)
    slots = jnp.arange(HOLD)
    live = slots[None, :] < counts[:, None]
    frames = jax.random.randint(jax.random.fold_in(key, 11), (N_SPACE * N_GRP, HOLD), F // 2, F + 1)
    return jnp.where(live, frames, 0).reshape(BLOCKS).astype(jnp.int32)


def draw_echoes(key, part):
    value_key = jax.random.fold_in(jax.random.fold_in(key, 3), 0)
    position = jnp.arange(BLOCKS, dtype=jnp.float32) / max(BLOCKS - 1, 1)
    scales = 3.0 ** position
    values = jnp.clip(jax.random.normal(value_key, (BLOCKS, F, V), jnp.float32), -6.0, 6.0)
    return (values * scales[:, None, None]).astype(jnp.bfloat16)


def with_ends(array, rng, low, high):
    shape = array.shape
    place = [jax.random.randint(jax.random.fold_in(rng, axis), (), 0, shape[axis]) for axis in range(len(shape))]
    array = array.at[tuple(place)].set(low)
    longest = shape.index(max(shape))
    place[longest] = (place[longest] + 1) % shape[longest]
    return array.at[tuple(place)].set(high)


def bell_draw(stream_key, dims, scale, limit, kind=jnp.bfloat16):
    result = scale * jax.random.normal(stream_key, dims, jnp.float32)
    return jnp.clip(result, min=-limit, max=limit).astype(kind)


def setup_inputs(seed: int = 0) -> dict:
    arg_keys = jax.random.split(jax.random.key(seed), 6)
    echoes = draw_echoes(jax.random.fold_in(arg_keys[5], 71), 0)
    frame_count = draw_frame_count(jax.random.fold_in(arg_keys[5], 71), 0)
    clutter_rank = with_ends(jax.random.randint(arg_keys[2], (BLOCKS,), 1, K // 4 + 1), jax.random.fold_in(arg_keys[2], 1), 1, (K // 4 + 1) - 1).astype(jnp.int32)
    noise_rank = with_ends(jax.random.randint(arg_keys[3], (BLOCKS,), K // 2, K + 1), jax.random.fold_in(arg_keys[3], 1), K // 2, K).astype(jnp.int32)
    start_basis = bell_draw(arg_keys[4], (F, K), 1.0, 6.0, jnp.float32)
    return {"echoes": echoes, "frame_count": frame_count, "clutter_rank": clutter_rank, "noise_rank": noise_rank, "start_basis": start_basis}


def filter_block(echo_block, frame_total, clutter_cut, noise_cut, initial):
    frames = jnp.arange(echo_block.shape[0], dtype=jnp.int32)
    frame_mask = (frames < frame_total).astype(jnp.bfloat16)
    padding_diag = (frames >= frame_total).astype(jnp.float32)
    masked = echo_block * frame_mask[:, None]
    gram_matrix = jnp.dot(masked.astype(jnp.float32), masked.T.astype(jnp.float32), preferred_element_type=jnp.float32) + jnp.diag(padding_diag)
    subspace = initial
    for iteration in range(ITERS):
        product = jnp.dot(gram_matrix, subspace, precision=lax.Precision.HIGHEST)
        inner_gram = jnp.dot(product.T, product, precision=lax.Precision.HIGHEST)
        factor = jnp.linalg.cholesky(inner_gram)
        subspace = jax.scipy.linalg.solve_triangular(factor, product.T, lower=True).T
    basis = subspace.astype(jnp.bfloat16)
    coefficients = jnp.dot(basis.T.astype(jnp.float32), masked.astype(jnp.float32), preferred_element_type=jnp.float32)
    columns = jnp.arange(basis.shape[1], dtype=jnp.int32)
    band_mask = ((columns >= clutter_cut) & (columns < noise_cut)).astype(jnp.float32)
    coefficients = (coefficients * band_mask[:, None]).astype(jnp.bfloat16)
    return jnp.dot(basis.astype(jnp.float32), coefficients.astype(jnp.float32), preferred_element_type=jnp.float32).astype(jnp.bfloat16)

def reference(echoes, frame_count, clutter_rank, noise_rank, start_basis):

    def one_block(block_items):
        return filter_block(block_items[0], block_items[1], block_items[2], block_items[3], start_basis)
    cleaned = lax.map(one_block, (echoes, frame_count, clutter_rank, noise_rank))
    width = cleaned.shape[2]
    half_width = width // 2
    window = jnp.sin(jnp.pi * (jnp.arange(width, dtype=jnp.float32) + 0.5) / width) ** 2
    upper_half = cleaned[:, :, half_width:].astype(jnp.float32) * window[half_width:]
    lower_half = cleaned[:, :, :half_width].astype(jnp.float32) * window[:half_width]
    following = jnp.concatenate([lower_half[1:], jnp.zeros_like(lower_half[:1])], axis=0)
    regions = upper_half + following
    frames_total = regions.shape[1]
    volume = jnp.transpose(regions, (1, 0, 2)).reshape(frames_total, -1)
    strength = jnp.sum(volume * volume, axis=0) / frames_total
    power = strength / (jnp.mean(strength) + 1e-06)
    return (volume, power)
```

```python
import functools
import numpy as np
import jax, jax.numpy as jnp
from jax import lax
from jax.experimental import pallas as pl
from jax.experimental.pallas import tpu as pltpu
from jax.sharding import PartitionSpec as P

F32, BF = jnp.float32, jnp.bfloat16
ITERS = 4
CHUNK = 512

NT = (((1,), (1,)), ((), ()))
NN = (((1,), (0,)), ((), ()))

def mm(a, b, dims):
    return lax.dot_general(a, b, dims, preferred_element_type=F32)

def split(a):
    hi = a.astype(BF)
    return hi, (a - hi.astype(F32)).astype(BF)

def split3(a):
    hi = a.astype(BF)
    rest = a - hi.astype(F32)
    mid = rest.astype(BF)
    return hi, mid, (rest - mid.astype(F32)).astype(BF)

def eliminate(a_ref, s_ref, blocks, k, w, between):
    tiles = k // 8
    sub = lax.broadcasted_iota(jnp.int32, (8, 128), 0)
    lane = lax.broadcasted_iota(jnp.int32, (8, 128), 1)
    for p in range(k // w):
        j0 = p * w
        t0, r0 = j0 // 8, j0 % 8
        inside = (lane >= j0) & (lane < j0 + w)
        between(p)
        cols, diag = {}, {}
        for b in blocks:
            for t in range(t0, tiles):
                tile = a_ref[b, 8 * t:8 * t + 8, :]
                for q in range(w):
                    cols[b, q, t] = jnp.broadcast_to(tile[:, j0 + q:j0 + q + 1], (8, 128))
                if t == t0:
                    diag[b] = jnp.where(inside, 0.0, tile)
        facs, rows, scal = {}, {}, {}
        for q in range(w):
            r, j = r0 + q, j0 + q
            for b in blocks:
                pivot = jnp.broadcast_to(cols[b, q, t0][r:r + 1, :], (8, 128))
                inv = 1.0 / pivot
                root = lax.rsqrt(pivot)
                scal[b] = root if q == 0 else jnp.where(sub == r, root, scal[b])
                for t in range(t0, tiles):
                    f = cols[b, q, t] * inv
                    facs[b, q, t] = jnp.where(sub > r, f, 0.0) if t == t0 else f
                for q2 in range(q + 1, w):
                    m = jnp.broadcast_to(cols[b, q2, t0][r:r + 1, :], (8, 128))
                    for t in range(t0, tiles):
                        cols[b, q2, t] = cols[b, q2, t] - facs[b, q, t] * m
                row = jnp.broadcast_to(diag[b][r:r + 1, :], (8, 128))
                row = jnp.where(lane == j, 1.0, jnp.where((lane > j) & (lane < j0 + w), 0.0, row))
                rows[b, q] = row
                diag[b] = diag[b] - facs[b, q, t0] * row
        for b in blocks:
            a_ref[b, 8 * t0:8 * t0 + 8, :] = diag[b]
            s_ref[b, j0:j0 + w, :] = scal[b][r0:r0 + w, :]
            for t in range(t0 + 1, tiles):
                tile = jnp.where(inside, 0.0, a_ref[b, 8 * t:8 * t + 8, :])
                for q in range(w):
                    tile = tile - facs[b, q, t] * rows[b, q]
                a_ref[b, 8 * t:8 * t + 8, :] = tile


def subspace_kernel(n, w, count_of, echo_ref, *refs):
    (fc_ref, cr_ref, nr_ref, start_ref, st_ref, s_out_ref, border_ref, x_ref, first_ref, gh_ref, gl_ref, p_ref, y_ref, a_ref, s_ref) = refs
    step = pl.program_id(0)
    frames, k = start_ref.shape
    lp = gh_ref.shape[2]

    @pl.when(step == 0)
    def _():
        x_ref[...] = jnp.zeros_like(x_ref)
        gh_ref[...] = jnp.zeros_like(gh_ref)
        gl_ref[...] = jnp.zeros_like(gl_ref)
        p_ref[...] = jnp.zeros_like(p_ref)
        y_ref[...] = jnp.zeros_like(y_ref)

    total = fc_ref[count_of(step)]
    row = lax.broadcasted_iota(jnp.int32, (frames, 1), 0)
    x_ref[:frames, :] = jnp.where(row < total, echo_ref[0], jnp.zeros((), BF))
    x = x_ref[...]
    g = mm(x[:-(-frames // 16) * 16], x, NT)

    @pl.when(step == 0)
    def _():
        first_ref[...] = x_ref[:, :first_ref.shape[1]]

    gr = lax.broadcasted_iota(jnp.int32, g.shape, 0)
    gc = lax.broadcasted_iota(jnp.int32, g.shape, 1)
    g = g + jnp.where((gr == gc) & (gr >= total) & (gr < frames), 1.0, 0.0)
    hi, lo = split(g)
    gh_ref[step, :g.shape[0], :] = hi
    gl_ref[step, :g.shape[0], :] = lo

    @pl.when(step == n - 1)
    def _():
        blocks = range(n)
        s0 = start_ref[...]
        s0 = jnp.concatenate([s0, jnp.zeros((frames, 128 - k), F32)], axis=1)
        s0 = jnp.concatenate([s0, jnp.zeros((lp - frames, 128), F32)], axis=0)
        s0t = s0.T
        sh, sl = split(s0t)
        for b in blocks:
            p_ref[b, :, :] = mm(sh, gh_ref[b], NN) + mm(sh, gl_ref[b], NN) + mm(sl, gh_ref[b], NN)

        def factor(between):
            for b in blocks:
                p = p_ref[b]
                h, m, l = split3(p)
                a_ref[b, :, :] = (mm(h[:k], h, NT) + (mm(h[:k], m, NT) + mm(m[:k], h, NT))
                                  + (mm(m[:k], m, NT) + mm(h[:k], l, NT) + mm(l[:k], h, NT)))
            eliminate(a_ref, s_ref, blocks, k, w, between)

        def inverse(b):
            lower = a_ref[b]
            ri = lax.broadcasted_iota(jnp.int32, lower.shape, 0)
            ci = lax.broadcasted_iota(jnp.int32, lower.shape, 1)
            lower = jnp.where(ci < ri, lower, jnp.where(ci == ri, 1.0, 0.0))
            return lower * s_ref[b]

        def body(i, carry):
            panels = k // w
            at = {panels * (b + 1) // (n + 1): b for b in blocks}

            def between(p):
                if p in at:
                    b = at[p]
                    ph, plo = split(p_ref[b, :k, :])
                    y_ref[b, :k, :] = mm(ph, gh_ref[b], NN) + mm(ph, gl_ref[b], NN) + mm(plo, gh_ref[b], NN)
            factor(between)
            for b in blocks:
                vh, vl = split(inverse(b))
                yh, yl = split(y_ref[b])
                p_ref[b, :k, :] = mm(vh, yh, NN) + mm(vh, yl, NN) + mm(vl, yh, NN)
            return carry

        lax.fori_loop(0, ITERS - 1, body, 0)
        factor(lambda p: None)
        for b in blocks:
            vh, vl = split(inverse(b))
            ph, plo = split(p_ref[b])
            st = mm(vh, ph, NN) + mm(vh, plo, NN) + mm(vl, ph, NN)
            st = jnp.concatenate([st, jnp.zeros((128 - k, lp), F32)], axis=0)
            st_ref[b, :, :] = st.astype(BF)
            s_out_ref[b, :, :] = st.T.astype(BF)
        slot = count_of(0)
        band = band_of(k, cr_ref[slot], nr_ref[slot])
        basis = st_ref[0, :k, :]
        border_ref[:, :lp] = basis
        border_ref[:, lp:] = (mm(basis, first_ref[...], NN) * band).astype(BF)


def subspace(echoes, fc, cr, nr, start, count_of, w=4):
    n, frames, width = echoes.shape
    k = start.shape[1]
    lp = -(-frames // 128) * 128
    smem = pl.BlockSpec(memory_space=pltpu.SMEM)
    edge = (k, lp + width // 2)
    return pl.pallas_call(
        functools.partial(subspace_kernel, n, w, count_of),
        grid=(n,),
        in_specs=[pl.BlockSpec((1, frames, width), lambda i: (i, 0, 0)),
                  smem, smem, smem,
                  pl.BlockSpec((frames, k), lambda i: (0, 0))],
        out_specs=[pl.BlockSpec((n, 128, lp), lambda i: (0, 0, 0)),
                   pl.BlockSpec((n, lp, 128), lambda i: (0, 0, 0)),
                   pl.BlockSpec(edge, lambda i: (0, 0))],
        out_shape=[jax.ShapeDtypeStruct((n, 128, lp), BF), jax.ShapeDtypeStruct((n, lp, 128), BF),
                   jax.ShapeDtypeStruct(edge, BF)],
        scratch_shapes=[pltpu.VMEM((lp, width), BF), pltpu.VMEM((lp, width // 2), BF), pltpu.VMEM((n, lp, lp), BF), pltpu.VMEM((n, lp, lp), BF),
                        pltpu.VMEM((n, 128, lp), F32), pltpu.VMEM((n, 128, lp), F32),
                        pltpu.VMEM((n, k, 128), F32), pltpu.VMEM((n, k, 128), F32)],
        compiler_params=pltpu.CompilerParams(vmem_limit_bytes=60 << 20),
        name="subspace",
    )(echoes, fc, cr, nr, start)


def project_kernel(n, count_of, echo_ref, st_ref, s_ref, fc_ref, cr_ref, nr_ref, win_ref, vol_ref, str_ref, last_ref,
                   x_ref, coef_ref, prev_ref):
    step = pl.program_id(0)
    frames, width = echo_ref.shape[1:]
    half = width // 2
    k = coef_ref.shape[0] - 32
    rows = prev_ref.shape[0]

    @pl.when(step == 0)
    def _():
        x_ref[...] = jnp.zeros_like(x_ref)
        coef_ref[...] = jnp.zeros_like(coef_ref)

    slot = count_of(step)
    total = fc_ref[slot]
    fr = lax.broadcasted_iota(jnp.int32, (frames, 1), 0)
    band = band_of(k, cr_ref[slot], nr_ref[slot])
    x_ref[:frames, :] = jnp.where(fr < total, echo_ref[0], jnp.zeros((), BF))
    st, s = st_ref[0, :k, :], s_ref[0, :rows, :]
    for c in range(width // CHUNK):
        at = slice(c * CHUNK, (c + 1) * CHUNK)
        coef_ref[:k, at] = (mm(st, x_ref[:, at], NN) * band).astype(BF)

    @pl.when(step > 0)
    def _():
        for c in range(half // CHUNK):
            at = slice(c * CHUNK, (c + 1) * CHUNK)
            low = mm(s, coef_ref[:, at], NN).astype(BF).astype(F32)
            vol = (prev_ref[:, at] + low * win_ref[:, at])[:frames]
            vol_ref[:, at] = vol
            str_ref[:, at] = jnp.sum(vol * vol, axis=0, keepdims=True) / frames

    for c in range(half // CHUNK):
        at, up = slice(c * CHUNK, (c + 1) * CHUNK), slice(half + c * CHUNK, half + (c + 1) * CHUNK)
        prev_ref[:, at] = mm(s, coef_ref[:, up], NN).astype(BF).astype(F32) * win_ref[:, up]

    @pl.when(step == n - 1)
    def _():
        last_ref[...] = prev_ref[...]


def band_of(k, low, high):
    col = lax.broadcasted_iota(jnp.int32, (k, 1), 0)
    return jnp.where((col >= low) & (col < high), 1.0, 0.0)


def project(echoes, st, s, fc, cr, nr, window, count_of):
    n, frames, width = echoes.shape
    half, lp, k = width // 2, st.shape[2], st.shape[1] - 32
    rows = -(-frames // 16) * 16
    smem = pl.BlockSpec(memory_space=pltpu.SMEM)
    after = lambda i: (0, jnp.maximum(i - 1, 0))
    return pl.pallas_call(
        functools.partial(project_kernel, n, count_of),
        grid=(n,),
        in_specs=[pl.BlockSpec((1, frames, width), lambda i: (i, 0, 0)),
                  pl.BlockSpec((1, 128, lp), lambda i: (i, 0, 0)),
                  pl.BlockSpec((1, lp, 128), lambda i: (i, 0, 0)),
                  smem, smem, smem,
                  pl.BlockSpec((1, width), lambda i: (0, 0))],
        out_specs=[pl.BlockSpec((frames, half), after), pl.BlockSpec((1, half), after),
                   pl.BlockSpec((rows, half), lambda i: (0, 0))],
        out_shape=[jax.ShapeDtypeStruct((frames, n * half), F32), jax.ShapeDtypeStruct((1, n * half), F32),
                   jax.ShapeDtypeStruct((rows, half), F32)],
        scratch_shapes=[pltpu.VMEM((lp, width), BF), pltpu.VMEM((k + 32, width), BF), pltpu.VMEM((rows, half), F32)],
        compiler_params=pltpu.CompilerParams(vmem_limit_bytes=40 << 20),
        cost_estimate=pl.CostEstimate(flops=int(8e9), bytes_accessed=int(12e6), transcendentals=0),
        name="project",
    )(echoes, st, s, fc, cr, nr, window)


def border_kernel(n, border_ref, last_ref, win_ref, str_in_ref, vol_in_ref, vol_ref, str_ref, sum_ref, fac_ref):
    frames, half = vol_ref.shape
    rows = last_ref.shape[0]
    k = border_ref.shape[0]
    lp = border_ref.shape[1] - half
    fac_ref[k:, :] = jnp.zeros((128 - k, fac_ref.shape[1]), BF)
    fac_ref[:k, :] = border_ref[...]
    s = fac_ref[:, :lp].astype(F32).T.astype(BF)[:rows]
    done = (n - 1) * half
    parts = jnp.zeros((1, 128), F32)
    for c in range(done // 128):
        at = slice(c * 128, c * 128 + 128)
        parts = parts + str_in_ref[:, at]
    str_ref[:, :done] = str_in_ref[:, :done]
    for c in range(half // CHUNK):
        at = slice(c * CHUNK, (c + 1) * CHUNK)
        low = mm(s, fac_ref[:, lp + c * CHUNK:lp + (c + 1) * CHUNK], NN).astype(BF).astype(F32)
        vol = (last_ref[:, at] + low * win_ref[:, at])[:frames]
        vol_ref[:, at] = vol
        part = jnp.sum(vol * vol, axis=0, keepdims=True) / frames
        str_ref[:, done + c * CHUNK:done + (c + 1) * CHUNK] = part
        for d in range(CHUNK // 128):
            parts = parts + part[:, d * 128:d * 128 + 128]
    sum_ref[0] = parts


def finish(border, last, window, strength, volume, n):
    rows, half = last.shape
    frames = volume.shape[0]
    vm = pl.BlockSpec(memory_space=pltpu.VMEM)
    whole = lambda a: pl.BlockSpec(a.shape, lambda i: (0, 0))
    return pl.pallas_call(
        functools.partial(border_kernel, n),
        grid=(1,),
        in_specs=[whole(border), whole(last), whole(window), whole(strength), pl.BlockSpec(memory_space=pl.ANY)],
        out_specs=[pl.BlockSpec((frames, half), lambda i: (0, n - 1)), whole(strength),
                   pl.BlockSpec((1, 1, 128), lambda i: (0, 0, 0))],
        out_shape=[jax.ShapeDtypeStruct(volume.shape, F32), jax.ShapeDtypeStruct(strength.shape, F32),
                   jax.ShapeDtypeStruct((1, 1, 128), F32)],
        scratch_shapes=[pltpu.VMEM((128, border.shape[1]), BF)],
        input_output_aliases={4: 0},
        compiler_params=pltpu.CompilerParams(vmem_limit_bytes=40 << 20),
        name="finish",
    )(border, last, window, strength, volume)


def reduce_kernel(dims, in_ref, out_ref, near_ref, far_ref, mid_ref, send1, recv1, send2, recv2):
    ny, nz, nx, ng = dims
    plane = ny * nx * ng
    place, core = lax.axis_index("space"), lax.axis_index("grp")
    y, z, x = place // (nz * nx), (place // nx) % nz, place % nx
    me = (y * nx + x) * ng + core

    def near(j):
        other = (me + j) % plane
        return ((other // (nx * ng)) * nz * nx + z * nx + (other // ng) % nx, other % ng)

    def far(j):
        return (y * nz * nx + ((z + j) % nz) * nx + x, core)

    barrier = pltpu.get_barrier_semaphore()

    def greet(peer):
        def body(j, carry):
            pl.semaphore_signal(barrier, inc=1, device_id=peer(j), device_id_type=pl.DeviceIdType.MESH)
            return carry
        return body

    lax.fori_loop(1, plane, greet(near), 0)
    lax.fori_loop(1, nz, greet(far), 0)
    near_ref[me] = in_ref[0]
    pl.semaphore_wait(barrier, plane - 1 + nz - 1)

    def near_copy(j, slot, peer):
        return pltpu.make_async_remote_copy(
            src_ref=in_ref.at[0], dst_ref=near_ref.at[slot], send_sem=send1.at[j], recv_sem=recv1.at[slot],
            device_id=peer, device_id_type=pl.DeviceIdType.MESH)

    def far_copy(j, slot, peer):
        return pltpu.make_async_remote_copy(
            src_ref=mid_ref.at[0], dst_ref=far_ref.at[slot], send_sem=send2.at[j], recv_sem=recv2.at[slot],
            device_id=peer, device_id_type=pl.DeviceIdType.MESH)

    def near_start(j, carry):
        near_copy(j, me, near(j)).start()
        return carry

    def near_wait(j, carry):
        near_copy(j, (me + j) % plane, near(j)).wait()
        return carry

    def far_start(j, carry):
        far_copy(j, z, far(j)).start()
        return carry

    def far_wait(j, carry):
        far_copy(j, (z + j) % nz, far(j)).wait()
        return carry

    lax.fori_loop(1, plane, near_start, 0)
    lax.fori_loop(1, plane, near_wait, 0)
    part = jnp.sum(near_ref[...], axis=0)
    mid_ref[0] = part
    far_ref[z] = part
    lax.fori_loop(1, nz, far_start, 0)
    lax.fori_loop(1, nz, far_wait, 0)
    total = jnp.sum(jnp.sum(far_ref[...], axis=0), axis=1, keepdims=True)
    out_ref[...] = jnp.broadcast_to(total, out_ref.shape)


def total_of(parts, dims):
    ny, nz, nx, ng = dims
    plane = ny * nx * ng
    vm = pl.BlockSpec(memory_space=pltpu.VMEM)
    return pl.pallas_call(
        functools.partial(reduce_kernel, dims),
        in_specs=[vm],
        out_specs=vm,
        out_shape=jax.ShapeDtypeStruct((1, 128), F32),
        scratch_shapes=[pltpu.VMEM((plane, 1, 128), F32), pltpu.VMEM((nz, 1, 128), F32), pltpu.VMEM((1, 1, 128), F32),
                        pltpu.SemaphoreType.DMA((plane,)), pltpu.SemaphoreType.DMA((plane,)),
                        pltpu.SemaphoreType.DMA((nz,)), pltpu.SemaphoreType.DMA((nz,))],
        compiler_params=pltpu.CompilerParams(collective_id=0, has_side_effects=True),
        name="total",
    )(parts)


def shards(dims, echoes, frame_count, clutter_rank, noise_rank, start_basis):
    n, frames, width = echoes.shape
    half = width // 2
    devices = dims[0] * dims[1] * dims[2] * dims[3]
    spot = np.arange(width, dtype=np.float64)
    window = jnp.asarray((np.sin(np.pi * (spot + 0.5) / width) ** 2).astype(np.float32)[None])

    def slot_of(b):
        return (lax.axis_index("space") * dims[3] + lax.axis_index("grp")) * n + b

    st, s, border = subspace(echoes, frame_count, clutter_rank, noise_rank, start_basis, slot_of)
    back = [(d + 1, d) for d in range(devices - 1)]
    border = lax.ppermute(border, ("space", "grp"), back)
    volume, strength, last = project(echoes, st, s, frame_count, clutter_rank, noise_rank, window, slot_of)
    volume, strength, parts = finish(border, last, window, strength, volume, n)
    total = total_of(parts, dims)[0, 0]
    power = strength.reshape(-1) / (total / (devices * n * half) + 1e-6)
    return volume, power


def solution(mesh):
    dims = (4, 8, 4, mesh.shape["grp"])
    both = ("space", "grp")
    return jax.shard_map(
        functools.partial(shards, dims), mesh=mesh,
        in_specs=(P(both, None, None), P(), P(), P(), P()),
        out_specs=(P(None, both), P(both)), check_vma=False)
```

```python
import functools
import numpy as np
import jax, jax.numpy as jnp
from jax import lax
from jax.experimental import pallas as pl
from jax.experimental.pallas import tpu as pltpu
from jax.sharding import PartitionSpec as P

F32, BF = jnp.float32, jnp.bfloat16
ITERS = 4
CHUNK = 512

NT = (((1,), (1,)), ((), ()))
NN = (((1,), (0,)), ((), ()))

def mm(a, b, dims):
    return lax.dot_general(a, b, dims, preferred_element_type=F32)

def split(a):
    hi = a.astype(BF)
    return hi, (a - hi.astype(F32)).astype(BF)

def split3(a):
    hi = a.astype(BF)
    rest = a - hi.astype(F32)
    mid = rest.astype(BF)
    return hi, mid, (rest - mid.astype(F32)).astype(BF)

def spread(tile, row):
    return jnp.take_along_axis(tile, jnp.full((8, 128), row, jnp.int32), axis=0)


def eliminate(a_ref, s_ref, blocks, k, w, between):
    tiles = k // 8
    sub = lax.broadcasted_iota(jnp.int32, (8, 128), 0)
    lane = lax.broadcasted_iota(jnp.int32, (8, 128), 1)
    for p in range(k // w):
        j0 = p * w
        t0, r0 = j0 // 8, j0 % 8
        inside = (lane >= j0) & (lane < j0 + w)
        between(p)
        cols, diag, tile = {}, {}, {}
        for b in blocks:
            for t in range(t0, tiles):
                tile[b, t] = a_ref[b, 8 * t:8 * t + 8, :]
            diag[b] = jnp.where(inside, 0.0, tile[b, t0])
        for q in range(w):
            for b in blocks:
                for t in range(t0, tiles):
                    cols[b, q, t] = jnp.broadcast_to(tile[b, t][:, j0 + q:j0 + q + 1], (8, 128))
        facs, rows, scal = {}, {}, {}
        for q in range(w):
            r, j = r0 + q, j0 + q
            for b in blocks:
                pivot = spread(cols[b, q, t0], r)
                inv = 1.0 / pivot
                root = lax.rsqrt(pivot)
                scal[b] = root if q == 0 else jnp.where(sub == r, root, scal[b])
                for t in range(t0, tiles):
                    f = cols[b, q, t] * inv
                    facs[b, q, t] = jnp.where(sub > r, f, 0.0) if t == t0 else f
                for q2 in range(q + 1, w):
                    m = spread(cols[b, q2, t0], r)
                    for t in range(t0, tiles):
                        cols[b, q2, t] = cols[b, q2, t] - facs[b, q, t] * m
                row = spread(diag[b], r)
                row = jnp.where(lane == j, 1.0, jnp.where((lane > j) & (lane < j0 + w), 0.0, row))
                rows[b, q] = row
                diag[b] = diag[b] - facs[b, q, t0] * row
        for b in blocks:
            a_ref[b, 8 * t0:8 * t0 + 8, :] = diag[b]
            s_ref[b, j0:j0 + w, :] = scal[b][r0:r0 + w, :]
            for t in range(t0 + 1, tiles):
                rest = jnp.where(inside, 0.0, tile[b, t])
                for q in range(w):
                    rest = rest - facs[b, q, t] * rows[b, q]
                a_ref[b, 8 * t:8 * t + 8, :] = rest


def subspace_kernel(n, w, count_of, echo_ref, *refs):
    (fc_ref, cr_ref, nr_ref, start_ref, st_ref, s_out_ref, border_ref, x_ref, first_ref, gh_ref, gl_ref, p_ref, y_ref, a_ref, s_ref) = refs
    step = pl.program_id(0)
    k, frames = start_ref.shape
    lp = gh_ref.shape[2]

    @pl.when(step == 0)
    def _():
        top = frames // 16 * 16
        x_ref[top:, :] = jnp.zeros((lp - top, x_ref.shape[1]), BF)
        gh_ref[:, top:, :] = jnp.zeros((n, lp - top, lp), BF)
        gl_ref[:, top:, :] = jnp.zeros((n, lp - top, lp), BF)
        p_ref[0] = jnp.zeros_like(p_ref[0])
        p_ref[:, k:, :] = jnp.zeros((n, 128 - k, lp), F32)
        y_ref[:, k:, :] = jnp.zeros((n, 128 - k, lp), F32)

    total = fc_ref[count_of(step)]
    row = lax.broadcasted_iota(jnp.int32, (frames, 1), 0)
    x_ref[:frames, :] = jnp.where(row < total, echo_ref[0], jnp.zeros((), BF))
    x = x_ref[...]
    g = mm(x[:-(-frames // 16) * 16], x, NT)

    @pl.when(step == 0)
    def _():
        first_ref[...] = x_ref[:, :first_ref.shape[1]]

    gr = lax.broadcasted_iota(jnp.int32, g.shape, 0)
    gc = lax.broadcasted_iota(jnp.int32, g.shape, 1)
    g = g + jnp.where((gr == gc) & (gr >= total) & (gr < frames), 1.0, 0.0)
    hi, lo = split(g)
    gh_ref[step, :g.shape[0], :] = hi
    gl_ref[step, :g.shape[0], :] = lo

    @pl.when(step == n - 1)
    def _():
        blocks = range(n)
        p_ref[0, :k, :frames] = start_ref[...]
        sh, sl = split(p_ref[0])
        for b in blocks:
            p_ref[b, :, :] = mm(sh, gh_ref[b], NN) + mm(sh, gl_ref[b], NN) + mm(sl, gh_ref[b], NN)

        def factor(between):
            for b in blocks:
                p = p_ref[b]
                h, m, l = split3(p)
                a_ref[b, :, :] = (mm(h[:k], h, NT) + (mm(h[:k], m, NT) + mm(m[:k], h, NT))
                                  + (mm(m[:k], m, NT) + mm(h[:k], l, NT) + mm(l[:k], h, NT)))
            eliminate(a_ref, s_ref, blocks, k, w, between)

        def inverse(b):
            lower = a_ref[b]
            ri = lax.broadcasted_iota(jnp.int32, lower.shape, 0)
            ci = lax.broadcasted_iota(jnp.int32, lower.shape, 1)
            lower = jnp.where(ci < ri, lower, jnp.where(ci == ri, 1.0, 0.0))
            return lower * s_ref[b]

        def body(i, carry):
            panels = k // w
            at = {panels * (b + 1) // (n + 1): b for b in blocks}

            def between(p):
                if p in at:
                    b = at[p]
                    ph, plo = split(p_ref[b, :k, :])
                    y_ref[b, :k, :] = mm(ph, gh_ref[b], NN) + mm(ph, gl_ref[b], NN) + mm(plo, gh_ref[b], NN)
            factor(between)
            for b in blocks:
                vh, vl = split(inverse(b))
                yh, yl = split(y_ref[b])
                p_ref[b, :k, :] = mm(vh, yh, NN) + mm(vh, yl, NN) + mm(vl, yh, NN)
            return carry

        lax.fori_loop(0, ITERS - 1, body, 0)
        factor(lambda p: None)
        for b in blocks:
            vh, vl = split(inverse(b))
            ph, plo = split(p_ref[b])
            st = mm(vh, ph, NN) + mm(vh, plo, NN) + mm(vl, ph, NN)
            st = jnp.concatenate([st, jnp.zeros((128 - k, lp), F32)], axis=0)
            st_ref[b, :, :] = st.astype(BF)
            s_out_ref[b, :, :] = st.T.astype(BF)
        slot = count_of(0)
        band = band_of(k, cr_ref[slot], nr_ref[slot])
        basis = st_ref[0, :k, :]
        border_ref[:, :lp] = basis
        border_ref[:, lp:] = (mm(basis, first_ref[...], NN) * band).astype(BF)


def subspace(echoes, fc, cr, nr, start, count_of, w=4):
    n, frames, width = echoes.shape
    k = start.shape[0]
    lp = -(-frames // 128) * 128
    smem = pl.BlockSpec(memory_space=pltpu.SMEM)
    edge = (k, lp + width // 2)
    return pl.pallas_call(
        functools.partial(subspace_kernel, n, w, count_of),
        grid=(n,),
        in_specs=[pl.BlockSpec((1, frames, width), lambda i: (i, 0, 0)),
                  smem, smem, smem,
                  pl.BlockSpec((k, frames), lambda i: (0, 0))],
        out_specs=[pl.BlockSpec((n, 128, lp), lambda i: (0, 0, 0)),
                   pl.BlockSpec((n, lp, 128), lambda i: (0, 0, 0)),
                   pl.BlockSpec(edge, lambda i: (0, 0))],
        out_shape=[jax.ShapeDtypeStruct((n, 128, lp), BF), jax.ShapeDtypeStruct((n, lp, 128), BF),
                   jax.ShapeDtypeStruct(edge, BF)],
        scratch_shapes=[pltpu.VMEM((lp, width), BF), pltpu.VMEM((lp, width // 2), BF), pltpu.VMEM((n, lp, lp), BF), pltpu.VMEM((n, lp, lp), BF),
                        pltpu.VMEM((n, 128, lp), F32), pltpu.VMEM((n, 128, lp), F32),
                        pltpu.VMEM((n, k, 128), F32), pltpu.VMEM((n, k, 128), F32)],
        compiler_params=pltpu.CompilerParams(vmem_limit_bytes=60 << 20),
        name="subspace",
    )(echoes, fc, cr, nr, start)


def project_kernel(n, count_of, echo_ref, st_ref, s_ref, fc_ref, cr_ref, nr_ref, win_ref, vol_ref, str_ref, last_ref,
                   x_ref, coef_ref, prev_ref):
    step = pl.program_id(0)
    frames, width = echo_ref.shape[1:]
    half = width // 2
    k = coef_ref.shape[0] - 32
    rows = prev_ref.shape[0]

    @pl.when(step == 0)
    def _():
        x_ref[...] = jnp.zeros_like(x_ref)
        coef_ref[...] = jnp.zeros_like(coef_ref)

    slot = count_of(step)
    total = fc_ref[slot]
    fr = lax.broadcasted_iota(jnp.int32, (frames, 1), 0)
    band = band_of(k, cr_ref[slot], nr_ref[slot])
    x_ref[:frames, :] = jnp.where(fr < total, echo_ref[0], jnp.zeros((), BF))
    st, s = st_ref[0, :k, :], s_ref[0, :rows, :]
    for c in range(width // CHUNK):
        at = slice(c * CHUNK, (c + 1) * CHUNK)
        coef_ref[:k, at] = (mm(st, x_ref[:, at], NN) * band).astype(BF)

    @pl.when(step > 0)
    def _():
        for c in range(half // CHUNK):
            at = slice(c * CHUNK, (c + 1) * CHUNK)
            low = mm(s, coef_ref[:, at], NN).astype(BF).astype(F32)
            vol = (prev_ref[:, at] + low * win_ref[:, at])[:frames]
            vol_ref[:, at] = vol
            str_ref[:, at] = jnp.sum(vol * vol, axis=0, keepdims=True) / frames

    for c in range(half // CHUNK):
        at, up = slice(c * CHUNK, (c + 1) * CHUNK), slice(half + c * CHUNK, half + (c + 1) * CHUNK)
        prev_ref[:, at] = mm(s, coef_ref[:, up], NN).astype(BF).astype(F32) * win_ref[:, up]

    @pl.when(step == n - 1)
    def _():
        last_ref[...] = prev_ref[...]


def band_of(k, low, high):
    col = lax.broadcasted_iota(jnp.int32, (k, 1), 0)
    return jnp.where((col >= low) & (col < high), 1.0, 0.0)


def project(echoes, st, s, fc, cr, nr, window, count_of):
    n, frames, width = echoes.shape
    half, lp, k = width // 2, st.shape[2], st.shape[1] - 32
    rows = -(-frames // 16) * 16
    smem = pl.BlockSpec(memory_space=pltpu.SMEM)
    after = lambda i: (0, jnp.maximum(i - 1, 0))
    return pl.pallas_call(
        functools.partial(project_kernel, n, count_of),
        grid=(n,),
        in_specs=[pl.BlockSpec((1, frames, width), lambda i: (i, 0, 0)),
                  pl.BlockSpec((1, 128, lp), lambda i: (i, 0, 0)),
                  pl.BlockSpec((1, lp, 128), lambda i: (i, 0, 0)),
                  smem, smem, smem,
                  pl.BlockSpec((1, width), lambda i: (0, 0))],
        out_specs=[pl.BlockSpec((frames, half), after), pl.BlockSpec((1, half), after),
                   pl.BlockSpec((rows, half), lambda i: (0, 0))],
        out_shape=[jax.ShapeDtypeStruct((frames, n * half), F32), jax.ShapeDtypeStruct((1, n * half), F32),
                   jax.ShapeDtypeStruct((rows, half), F32)],
        scratch_shapes=[pltpu.VMEM((lp, width), BF), pltpu.VMEM((k + 32, width), BF), pltpu.VMEM((rows, half), F32)],
        compiler_params=pltpu.CompilerParams(vmem_limit_bytes=62 << 20),
        cost_estimate=pl.CostEstimate(flops=int(8e9), bytes_accessed=int(12e6), transcendentals=0),
        name="project",
    )(echoes, st, s, fc, cr, nr, window)


def border_kernel(n, border_ref, last_ref, win_ref, str_in_ref, vol_in_ref, vol_ref, str_ref, sum_ref, fac_ref):
    frames, half = vol_ref.shape
    rows = last_ref.shape[0]
    k = border_ref.shape[0]
    lp = border_ref.shape[1] - half
    fac_ref[k:, :] = jnp.zeros((128 - k, fac_ref.shape[1]), BF)
    fac_ref[:k, :] = border_ref[...]
    s = fac_ref[:, :lp].astype(F32).T.astype(BF)[:rows]
    done = (n - 1) * half
    parts = jnp.zeros((1, 128), F32)
    for c in range(done // 128):
        at = slice(c * 128, c * 128 + 128)
        parts = parts + str_in_ref[:, at]
    str_ref[:, :done] = str_in_ref[:, :done]
    for c in range(half // CHUNK):
        at = slice(c * CHUNK, (c + 1) * CHUNK)
        low = mm(s, fac_ref[:, lp + c * CHUNK:lp + (c + 1) * CHUNK], NN).astype(BF).astype(F32)
        vol = (last_ref[:, at] + low * win_ref[:, at])[:frames]
        vol_ref[:, at] = vol
        part = jnp.sum(vol * vol, axis=0, keepdims=True) / frames
        str_ref[:, done + c * CHUNK:done + (c + 1) * CHUNK] = part
        for d in range(CHUNK // 128):
            parts = parts + part[:, d * 128:d * 128 + 128]
    sum_ref[0] = parts


def finish(border, last, window, strength, volume, n):
    rows, half = last.shape
    frames = volume.shape[0]
    vm = pl.BlockSpec(memory_space=pltpu.VMEM)
    whole = lambda a: pl.BlockSpec(a.shape, lambda i: (0, 0))
    return pl.pallas_call(
        functools.partial(border_kernel, n),
        grid=(1,),
        in_specs=[whole(border), whole(last), whole(window), whole(strength), pl.BlockSpec(memory_space=pl.ANY)],
        out_specs=[pl.BlockSpec((frames, half), lambda i: (0, n - 1)), whole(strength),
                   pl.BlockSpec((1, 1, 128), lambda i: (0, 0, 0))],
        out_shape=[jax.ShapeDtypeStruct(volume.shape, F32), jax.ShapeDtypeStruct(strength.shape, F32),
                   jax.ShapeDtypeStruct((1, 1, 128), F32)],
        scratch_shapes=[pltpu.VMEM((128, border.shape[1]), BF)],
        input_output_aliases={4: 0},
        compiler_params=pltpu.CompilerParams(vmem_limit_bytes=40 << 20),
        name="finish",
    )(border, last, window, strength, volume)


def reduce_kernel(dims, in_ref, out_ref, near_ref, far_ref, mid_ref, send1, recv1, send2, recv2):
    ny, nz, nx, ng = dims
    plane = ny * nx * ng
    place, core = lax.axis_index("space"), lax.axis_index("grp")
    y, z, x = place // (nz * nx), (place // nx) % nz, place % nx
    me = (y * nx + x) * ng + core

    def near(j):
        other = (me + j) % plane
        return ((other // (nx * ng)) * nz * nx + z * nx + (other // ng) % nx, other % ng)

    def far(j):
        return (y * nz * nx + ((z + j) % nz) * nx + x, core)

    barrier = pltpu.get_barrier_semaphore()

    def greet(peer):
        def body(j, carry):
            pl.semaphore_signal(barrier, inc=1, device_id=peer(j), device_id_type=pl.DeviceIdType.MESH)
            return carry
        return body

    lax.fori_loop(1, plane, greet(near), 0)
    lax.fori_loop(1, nz, greet(far), 0)
    near_ref[me] = in_ref[0]
    pl.semaphore_wait(barrier, plane - 1 + nz - 1)

    def near_copy(j, slot, peer):
        return pltpu.make_async_remote_copy(
            src_ref=in_ref.at[0], dst_ref=near_ref.at[slot], send_sem=send1.at[j], recv_sem=recv1.at[slot],
            device_id=peer, device_id_type=pl.DeviceIdType.MESH)

    def far_copy(j, slot, peer):
        return pltpu.make_async_remote_copy(
            src_ref=mid_ref.at[0], dst_ref=far_ref.at[slot], send_sem=send2.at[j], recv_sem=recv2.at[slot],
            device_id=peer, device_id_type=pl.DeviceIdType.MESH)

    def near_start(j, carry):
        near_copy(j, me, near(j)).start()
        return carry

    def near_wait(j, carry):
        near_copy(j, (me + j) % plane, near(j)).wait()
        return carry

    def far_start(j, carry):
        far_copy(j, z, far(j)).start()
        return carry

    def far_wait(j, carry):
        far_copy(j, (z + j) % nz, far(j)).wait()
        return carry

    lax.fori_loop(1, plane, near_start, 0)
    lax.fori_loop(1, plane, near_wait, 0)
    part = jnp.sum(near_ref[...], axis=0)
    mid_ref[0] = part
    far_ref[z] = part
    lax.fori_loop(1, nz, far_start, 0)
    lax.fori_loop(1, nz, far_wait, 0)
    total = jnp.sum(jnp.sum(far_ref[...], axis=0), axis=1, keepdims=True)
    out_ref[...] = jnp.broadcast_to(total, out_ref.shape)


def total_of(parts, dims):
    ny, nz, nx, ng = dims
    plane = ny * nx * ng
    vm = pl.BlockSpec(memory_space=pltpu.VMEM)
    return pl.pallas_call(
        functools.partial(reduce_kernel, dims),
        in_specs=[vm],
        out_specs=vm,
        out_shape=jax.ShapeDtypeStruct((1, 128), F32),
        scratch_shapes=[pltpu.VMEM((plane, 1, 128), F32), pltpu.VMEM((nz, 1, 128), F32), pltpu.VMEM((1, 1, 128), F32),
                        pltpu.SemaphoreType.DMA((plane,)), pltpu.SemaphoreType.DMA((plane,)),
                        pltpu.SemaphoreType.DMA((nz,)), pltpu.SemaphoreType.DMA((nz,))],
        compiler_params=pltpu.CompilerParams(collective_id=0, has_side_effects=True),
        name="total",
    )(parts)


def shards(dims, echoes, frame_count, clutter_rank, noise_rank, start_basis):
    n, frames, width = echoes.shape
    half = width // 2
    devices = dims[0] * dims[1] * dims[2] * dims[3]
    spot = np.arange(width, dtype=np.float64)
    window = jnp.asarray((np.sin(np.pi * (spot + 0.5) / width) ** 2).astype(np.float32)[None])

    def slot_of(b):
        return (lax.axis_index("space") * dims[3] + lax.axis_index("grp")) * n + b

    st, s, border = subspace(echoes, frame_count, clutter_rank, noise_rank, start_basis.T, slot_of)
    back = [(d + 1, d) for d in range(devices - 1)]
    border = lax.ppermute(border, ("space", "grp"), back)
    volume, strength, last = project(echoes, st, s, frame_count, clutter_rank, noise_rank, window, slot_of)
    volume, strength, parts = finish(border, last, window, strength, volume, n)
    total = total_of(parts, dims)[0, 0]
    power = strength.reshape(-1) / (total / (devices * n * half) + 1e-6)
    return volume, power


def solution(mesh):
    dims = (4, 8, 4, mesh.shape["grp"])
    both = ("space", "grp")
    return jax.shard_map(
        functools.partial(shards, dims), mesh=mesh,
        in_specs=(P(both, None, None), P(), P(), P(), P()),
        out_specs=(P(None, both), P(both)), check_vma=False)
```

```python
import functools
import numpy as np
import jax, jax.numpy as jnp
from jax import lax
from jax.experimental import pallas as pl
from jax.experimental.pallas import tpu as pltpu
from jax.sharding import PartitionSpec as P

F32, BF = jnp.float32, jnp.bfloat16
ITERS = 4
CHUNK = 512
EARLY = 0

NT = (((1,), (1,)), ((), ()))
NN = (((1,), (0,)), ((), ()))

def mm(a, b, dims):
    return lax.dot_general(a, b, dims, preferred_element_type=F32)

def split(a):
    hi = a.astype(BF)
    return hi, (a - hi.astype(F32)).astype(BF)

def split3(a):
    hi = a.astype(BF)
    rest = a - hi.astype(F32)
    mid = rest.astype(BF)
    return hi, mid, (rest - mid.astype(F32)).astype(BF)

def spread(tile, row):
    return jnp.take_along_axis(tile, jnp.full((8, 128), row, jnp.int32), axis=0)


GAP = 64


def eliminate(m_ref, s_ref, pairs, k, between):
    tiles = k // 8
    sub = lax.broadcasted_iota(jnp.int32, (8, 128), 0)
    place = lax.broadcasted_iota(jnp.int32, (8, 128), 1)
    lane = place & (GAP - 1)
    for p in range(tiles):
        j0 = 8 * p
        inside = (lane >= j0) & (lane < j0 + 8)
        eye = jnp.where(lane == j0 + sub, 1.0, 0.0)
        between(p)
        cols, diag, tile, inverses, pivots = {}, {}, {}, {}, {}
        for b in pairs:
            for t in range(p, tiles):
                tile[b, t] = m_ref[b, 8 * t:8 * t + 8, :]
            diag[b] = jnp.where(inside, eye, tile[b, p])
        for q in range(8):
            pick = place - lane + (j0 + q)
            for b in pairs:
                for t in range(p, tiles):
                    cols[b, q, t] = jnp.take_along_axis(tile[b, t], pick, axis=1)
        for q in range(8):
            for b in pairs:
                pivot = spread(cols[b, q, p], q)
                inv = 1.0 / pivot
                pivots[b] = pivot if q == 0 else jnp.where(sub == q, pivot, pivots[b])
                inverses[b] = inv if q == 0 else jnp.where(sub == q, inv, inverses[b])
                if q < 7:
                    f = jnp.where(sub > q, cols[b, q, p] * inv, 0.0)
                    for q2 in range(q + 1, 8):
                        cols[b, q2, p] = cols[b, q2, p] - f * spread(cols[b, q2, p], q)
                    diag[b] = diag[b] - f * spread(diag[b], q)
        for b in pairs:
            m_ref[b, j0:j0 + 8, :] = diag[b]
            s_ref[b, j0:j0 + 8, :] = lax.rsqrt(pivots[b])
        if p == tiles - 1:
            break
        for b in pairs:
            solved = diag[b] * inverses[b]
            for q in range(7, 0, -1):
                g = jnp.where(sub < q, cols[b, q, p] * inverses[b], 0.0)
                solved = solved - g * spread(solved, q)
            rows = [spread(solved, q) for q in range(8)]
            for t in range(p + 1, tiles):
                rest = jnp.where(inside, 0.0, tile[b, t])
                for q in range(8):
                    rest = rest - cols[b, q, t] * rows[q]
                m_ref[b, 8 * t:8 * t + 8, :] = rest


def mm3(a, b, dims=NN):
    (ah, al), (bh, bl) = a, b
    m = ah.shape[0]
    first = mm(jnp.concatenate([ah, al], axis=0), bh, dims)
    return first[:m] + (first[m:] + mm(ah, bl, dims))


def mm6(a, b, dims=NN):
    (ah, am, al), (bh, bm, bl) = a, b
    m = ah.shape[0]
    first = mm(jnp.concatenate([ah, am, al], axis=0), bh, dims)
    second = mm(jnp.concatenate([ah, am], axis=0), bm, dims)
    return first[:m] + (first[m:2 * m] + second[:m]) + (second[m:] + first[2 * m:] + mm(ah, bl, dims))


def both(parts, h):
    return tuple(jnp.concatenate([a[:h], a[GAP:GAP + h]], axis=0) for a in parts)


def chosen(rows, h):
    lane = lax.broadcasted_iota(jnp.int32, (h, 128), 1)
    return jnp.where(lane < GAP, rows[:h], rows[h:])


def stacked(x, pad):
    lane = lax.broadcasted_iota(jnp.int32, x.shape, 1)
    first, second = jnp.where(lane < GAP, x, 0.0), jnp.where(lane < GAP, 0.0, x)
    if not pad:
        return jnp.concatenate([first, second], axis=0)
    zero = jnp.zeros((pad, 128), F32)
    return jnp.concatenate([first, zero, second, zero], axis=0)


def subspace_kernel(n, count_of, echo_ref, *refs):
    (fc_ref, cr_ref, nr_ref, start_ref, st_ref, s_out_ref, border_ref, x_ref, gh_ref, gl_ref, p_ref, y_ref, a_ref, s_ref) = refs
    step = pl.program_id(0)
    k, frames = start_ref.shape
    lp = gh_ref.shape[2]

    @pl.when(step == 0)
    def _():
        top = frames // 16 * 16
        gh_ref[:, top:, :] = jnp.zeros((n, lp - top, lp), BF)
        gl_ref[:, top:, :] = jnp.zeros((n, lp - top, lp), BF)

    total = fc_ref[count_of(step)]
    row = lax.broadcasted_iota(jnp.int32, (frames, 1), 0)
    top = frames // 16 * 16
    x_ref[step, top:, :] = jnp.zeros((lp - top, x_ref.shape[2]), BF)
    x_ref[step, :frames, :] = jnp.where(row < total, echo_ref[0], jnp.zeros((), BF))
    x = x_ref[step]
    rows, cut = -(-frames // 16) * 16, frames // 256 * 256
    left = mm(x[:rows], x[:cut], NT)
    right = mm(x[cut:rows], x[cut:lp], NT)
    low = jnp.concatenate([left[cut:], jnp.zeros((lp - rows, cut), F32)], axis=0)
    g = jnp.concatenate([left, jnp.concatenate([low.T, right], axis=0)], axis=1)


    gr = lax.broadcasted_iota(jnp.int32, g.shape, 0)
    gc = lax.broadcasted_iota(jnp.int32, g.shape, 1)
    g = g + jnp.where((gr == gc) & (gr >= total) & (gr < frames), 1.0, 0.0)
    hi, lo = split(g)
    gh_ref[step, :g.shape[0], :] = hi
    gl_ref[step, :g.shape[0], :] = lo

    @pl.when(step == n - 1)
    def _():
        blocks = range(n)
        half = k // 2
        pairs = [(b, min(b + 1, n - 1)) for b in range(0, n, 2)]
        spots = [[(i, e * GAP) for i, pair in enumerate(pairs) for e in (0, 1) if pair[e] == b] for b in range(n)]

        def place(ref, b, value):
            for i, at in spots[b]:
                ref[i, 0, at:at + half, :] = value[:half]
                ref[i, 1, at:at + half, :] = value[half:]

        y_ref[0, 0, :, :] = jnp.zeros((128, lp), F32)
        y_ref[0, 0, :k, :frames] = start_ref[...]
        start = split(y_ref[0, 0])
        y_ref[...] = jnp.zeros_like(y_ref)
        p_ref[...] = jnp.zeros_like(p_ref)
        for b in range(n):
            place(p_ref, b, mm3(start, (gh_ref[b], gl_ref[b]))[:k])

        def forward(b):
            i, at = spots[b][0]
            p = jnp.concatenate([p_ref[i, 0, at:at + half, :], p_ref[i, 1, at:at + half, :]], axis=0)
            place(y_ref, b, mm3(split(p), (gh_ref[b], gl_ref[b])))

        count = range(len(pairs))

        def leaf(mats, between):
            for i in count:
                a_ref[i, :, :] = mats[i]
            eliminate(a_ref, s_ref, count, half, between)
            out = []
            for i in count:
                lower = a_ref[i]
                ri = lax.broadcasted_iota(jnp.int32, lower.shape, 0)
                ci = lax.broadcasted_iota(jnp.int32, lower.shape, 1) & (GAP - 1)
                out.append(jnp.where(ci < ri, lower, jnp.where(ci == ri, 1.0, 0.0)) * s_ref[i])
            return out

        def inverse(moves):
            z = [[split3(p_ref[i, 0]), split3(p_ref[i, 1])] for i in count]
            c11 = [chosen(mm6(both(z[i][0], half), z[i][0], NT), half) for i in count]
            c12, c22 = {}, {}

            def others(i):
                rows = tuple(jnp.concatenate(parts, axis=0) for parts in zip(both(z[i][0], half), both(z[i][1], half)))
                c = mm6(rows, z[i][1], NT)
                c12[i], c22[i] = chosen(c[:k], half), chosen(c[k:], half)

            panels = half // 8
            first = [functools.partial(others, i) for i in count] + moves[:EARLY]

            def run(some, last):
                plan = {}
                for e, m in enumerate(some):
                    plan.setdefault(e * last // max(len(some), 1), []).append(m)
                return lambda p: [m() for m in plan.get(p, [])]

            w11 = leaf(c11, run(first, panels - 1))
            fill = jnp.zeros((128 - half, 128), F32)
            u, ut = [], []
            for i in count:
                x = mm6(split3(w11[i]), split3(stacked(c12[i], GAP - half)))
                x = jnp.concatenate([x, fill], axis=0)
                u.append(x)
                ut.append(both(split3(x.T), half))
            w22 = leaf([c22[i] - chosen(mm6(ut[i], split3(u[i])), half) for i in count],
                       run(moves[EARLY:], panels - 1))
            out = []
            for i in count:
                t = chosen(mm3(ut[i][:2], split(jnp.concatenate([w11[i], fill], axis=0))), half)
                w21 = -mm3(split(w22[i]), split(stacked(t, GAP - half)))
                top = jnp.concatenate([stacked(w11[i], 0), jnp.zeros((k, 128), F32)], axis=1)
                low = jnp.concatenate([stacked(w21, 0), stacked(w22[i], 0)], axis=1)
                out.append(split(jnp.concatenate([top, low], axis=0)))
            return out

        def apply(factors, ref, i):
            rows = mm3(factors, split(jnp.concatenate([ref[i, 0], ref[i, 1]], axis=0)))
            return rows[:k], rows[k:]

        def body(i, carry):
            factors = inverse([functools.partial(forward, b) for b in range(n)])
            for i in count:
                top, low = apply(factors[i], y_ref, i)
                for e in (0, 1):
                    p_ref[i, 0, e * GAP:e * GAP + half, :] = top[e * half:(e + 1) * half]
                    p_ref[i, 1, e * GAP:e * GAP + half, :] = low[e * half:(e + 1) * half]
            return carry

        lax.fori_loop(0, ITERS - 1, body, 0)
        factors = inverse([])
        fill = jnp.zeros((128 - k, lp), F32)
        for i in count:
            top, low = apply(factors[i], p_ref, i)
            for e in (0, 1):
                b = pairs[i][e]
                if spots[b][0] == (i, e * GAP):
                    rows = slice(e * half, (e + 1) * half)
                    st = jnp.concatenate([top[rows], low[rows], fill], axis=0)
                    st_ref[b, :, :] = st.astype(BF)
                    s_out_ref[b, :, :] = st.T.astype(BF)
        slot = count_of(0)
        band = band_of(k, cr_ref[slot], nr_ref[slot])
        basis = st_ref[0, :k, :]
        border_ref[:, :lp] = basis
        border_ref[:, lp:] = (mm(basis, x_ref[0, :, :x_ref.shape[2] // 2], NN) * band).astype(BF)


def subspace(echoes, fc, cr, nr, start, count_of):
    n, frames, width = echoes.shape
    k = start.shape[0]
    lp = -(-frames // 128) * 128
    half_n = -(-n // 2)
    smem = pl.BlockSpec(memory_space=pltpu.SMEM)
    edge = (k, lp + width // 2)
    return pl.pallas_call(
        functools.partial(subspace_kernel, n, count_of),
        grid=(n,),
        in_specs=[pl.BlockSpec((1, frames, width), lambda i: (i, 0, 0)),
                  smem, smem, smem,
                  pl.BlockSpec((k, frames), lambda i: (0, 0))],
        out_specs=[pl.BlockSpec((n, 128, lp), lambda i: (0, 0, 0)),
                   pl.BlockSpec((n, lp, 128), lambda i: (0, 0, 0)),
                   pl.BlockSpec(edge, lambda i: (0, 0)),
                   pl.BlockSpec((n, lp, width), lambda i: (0, 0, 0))],
        out_shape=[jax.ShapeDtypeStruct((n, 128, lp), BF), jax.ShapeDtypeStruct((n, lp, 128), BF),
                   jax.ShapeDtypeStruct(edge, BF), jax.ShapeDtypeStruct((n, lp, width), BF)],
        scratch_shapes=[pltpu.VMEM((n, lp, lp), BF), pltpu.VMEM((n, lp, lp), BF),
                        pltpu.VMEM((half_n, 2, 128, lp), F32), pltpu.VMEM((half_n, 2, 128, lp), F32),
                        pltpu.VMEM((half_n, k // 2, 128), F32), pltpu.VMEM((half_n, k // 2, 128), F32)],
        compiler_params=pltpu.CompilerParams(vmem_limit_bytes=32 << 20),
        name="subspace",
    )(echoes, fc, cr, nr, start)


def project_kernel(n, frames, count_of, x_ref, st_ref, s_ref, cr_ref, nr_ref, win_ref, vol_ref, str_ref, last_ref,
                   coef_ref, prev_ref):
    step = pl.program_id(0)
    width = x_ref.shape[2]
    half = width // 2
    k = coef_ref.shape[0] - 32
    rows = prev_ref.shape[0]

    @pl.when(step == 0)
    def _():
        coef_ref[...] = jnp.zeros_like(coef_ref)

    slot = count_of(step)
    band = band_of(k, cr_ref[slot], nr_ref[slot])
    st, s = st_ref[0, :k, :], s_ref[0, :rows, :]
    for c in range(width // CHUNK):
        at = slice(c * CHUNK, (c + 1) * CHUNK)
        coef_ref[:k, at] = (mm(st, x_ref[0, :, at], NN) * band).astype(BF)

    @pl.when(step > 0)
    def _():
        for c in range(half // CHUNK):
            at = slice(c * CHUNK, (c + 1) * CHUNK)
            low = mm(s, coef_ref[:, at], NN).astype(BF).astype(F32)
            vol = (prev_ref[:, at] + low * win_ref[:, at])[:frames]
            vol_ref[:, at] = vol
            str_ref[:, at] = jnp.sum(vol * vol, axis=0, keepdims=True) / frames

    for c in range(half // CHUNK):
        at, up = slice(c * CHUNK, (c + 1) * CHUNK), slice(half + c * CHUNK, half + (c + 1) * CHUNK)
        prev_ref[:, at] = mm(s, coef_ref[:, up], NN).astype(BF).astype(F32) * win_ref[:, up]

    @pl.when(step == n - 1)
    def _():
        last_ref[...] = prev_ref[...]


def band_of(k, low, high):
    col = lax.broadcasted_iota(jnp.int32, (k, 1), 0)
    return jnp.where((col >= low) & (col < high), 1.0, 0.0)


def project(masked, frames, st, s, cr, nr, window, count_of):
    n, _, width = masked.shape
    half, lp, k = width // 2, st.shape[2], st.shape[1] - 32
    rows = -(-frames // 16) * 16
    smem = pl.BlockSpec(memory_space=pltpu.SMEM)
    after = lambda i: (0, jnp.maximum(i - 1, 0))
    return pl.pallas_call(
        functools.partial(project_kernel, n, frames, count_of),
        grid=(n,),
        in_specs=[pl.BlockSpec((1, lp, width), lambda i: (i, 0, 0)),
                  pl.BlockSpec((1, 128, lp), lambda i: (i, 0, 0)),
                  pl.BlockSpec((1, lp, 128), lambda i: (i, 0, 0)),
                  smem, smem,
                  pl.BlockSpec((1, width), lambda i: (0, 0))],
        out_specs=[pl.BlockSpec((frames, half), after), pl.BlockSpec((1, half), after),
                   pl.BlockSpec((rows, half), lambda i: (0, 0))],
        out_shape=[jax.ShapeDtypeStruct((frames, n * half), F32), jax.ShapeDtypeStruct((1, n * half), F32),
                   jax.ShapeDtypeStruct((rows, half), F32)],
        scratch_shapes=[pltpu.VMEM((k + 32, width), BF), pltpu.VMEM((rows, half), F32)],
        compiler_params=pltpu.CompilerParams(vmem_limit_bytes=32 << 20),
        cost_estimate=pl.CostEstimate(flops=int(8e9), bytes_accessed=int(12e6), transcendentals=0),
        name="project",
    )(masked, st, s, cr, nr, window)


def border_kernel(n, border_ref, last_ref, win_ref, str_in_ref, vol_in_ref, vol_ref, str_ref, sum_ref, fac_ref):
    frames, half = vol_ref.shape
    rows = last_ref.shape[0]
    k = border_ref.shape[0]
    lp = border_ref.shape[1] - half
    fac_ref[k:, :] = jnp.zeros((128 - k, fac_ref.shape[1]), BF)
    fac_ref[:k, :] = border_ref[...]
    s = fac_ref[:, :lp].astype(F32).T.astype(BF)[:rows]
    done = (n - 1) * half
    parts = jnp.zeros((1, 128), F32)
    for c in range(done // 128):
        at = slice(c * 128, c * 128 + 128)
        parts = parts + str_in_ref[:, at]
    str_ref[:, :done] = str_in_ref[:, :done]
    for c in range(half // CHUNK):
        at = slice(c * CHUNK, (c + 1) * CHUNK)
        low = mm(s, fac_ref[:, lp + c * CHUNK:lp + (c + 1) * CHUNK], NN).astype(BF).astype(F32)
        vol = (last_ref[:, at] + low * win_ref[:, at])[:frames]
        vol_ref[:, at] = vol
        part = jnp.sum(vol * vol, axis=0, keepdims=True) / frames
        str_ref[:, done + c * CHUNK:done + (c + 1) * CHUNK] = part
        for d in range(CHUNK // 128):
            parts = parts + part[:, d * 128:d * 128 + 128]
    sum_ref[0] = parts


def finish(border, last, window, strength, volume, n):
    rows, half = last.shape
    frames = volume.shape[0]
    vm = pl.BlockSpec(memory_space=pltpu.VMEM)
    whole = lambda a: pl.BlockSpec(a.shape, lambda i: (0, 0))
    return pl.pallas_call(
        functools.partial(border_kernel, n),
        grid=(1,),
        in_specs=[whole(border), whole(last), whole(window), whole(strength), pl.BlockSpec(memory_space=pl.ANY)],
        out_specs=[pl.BlockSpec((frames, half), lambda i: (0, n - 1)), whole(strength),
                   pl.BlockSpec((1, 1, 128), lambda i: (0, 0, 0))],
        out_shape=[jax.ShapeDtypeStruct(volume.shape, F32), jax.ShapeDtypeStruct(strength.shape, F32),
                   jax.ShapeDtypeStruct((1, 1, 128), F32)],
        scratch_shapes=[pltpu.VMEM((128, border.shape[1]), BF)],
        input_output_aliases={4: 0},
        compiler_params=pltpu.CompilerParams(vmem_limit_bytes=32 << 20),
        name="finish",
    )(border, last, window, strength, volume)


def reduce_kernel(dims, in_ref, out_ref, near_ref, far_ref, mid_ref, send1, recv1, send2, recv2):
    ny, nz, nx, ng = dims
    plane = ny * nx * ng
    place, core = lax.axis_index("space"), lax.axis_index("grp")
    y, z, x = place // (nz * nx), (place // nx) % nz, place % nx
    me = (y * nx + x) * ng + core

    hop = lambda step, size: min(step, size - step)
    steps = sorted(((dy, dx, dg) for dy in range(ny) for dx in range(nx) for dg in range(ng)),
                   key=lambda d: -hop(d[0], ny) - hop(d[1], nx))
    steps = [d for d in steps if d != (0, 0, 0)]
    ys = [(y + d) % ny for d in range(ny)]
    xs = [(x + d) % nx for d in range(nx)]
    gs = [(core + d) % ng for d in range(ng)]
    zs = [(z + d) % nz for d in range(nz)]
    near = [((ys[dy] * nz + z) * nx + xs[dx], gs[dg]) for dy, dx, dg in steps]
    slots = [(ys[dy] * nx + xs[dx]) * ng + gs[dg] for dy, dx, dg in steps]
    reach = sorted(range(1, nz), key=lambda d: -hop(d, nz))
    far = [((y * nz + zs[d]) * nx + x, core) for d in reach]

    barrier = pltpu.get_barrier_semaphore()
    for peer in far + near:
        pl.semaphore_signal(barrier, inc=1, device_id=peer, device_id_type=pl.DeviceIdType.MESH)
    near_ref[me] = in_ref[0]
    pl.semaphore_wait(barrier, len(near) + len(far))

    def near_copy(j, slot):
        return pltpu.make_async_remote_copy(
            src_ref=in_ref.at[0], dst_ref=near_ref.at[slot], send_sem=send1.at[j], recv_sem=recv1.at[slot],
            device_id=near[j], device_id_type=pl.DeviceIdType.MESH)

    def far_copy(j, slot):
        return pltpu.make_async_remote_copy(
            src_ref=mid_ref.at[0], dst_ref=far_ref.at[slot], send_sem=send2.at[j], recv_sem=recv2.at[slot],
            device_id=far[j], device_id_type=pl.DeviceIdType.MESH)

    for j in range(len(near)):
        near_copy(j, me).start()
    for j in range(len(near)):
        near_copy(j, slots[j]).wait_recv()
    part = jnp.sum(near_ref[...], axis=0)
    mid_ref[0] = part
    far_ref[z] = part
    for j in range(len(far)):
        far_copy(j, z).start()
    for j in range(len(near)):
        near_copy(j, me).wait_send()
    for j in range(len(far)):
        far_copy(j, zs[reach[j]]).wait_recv()
    total = jnp.sum(jnp.sum(far_ref[...], axis=0), axis=1, keepdims=True)
    out_ref[...] = jnp.broadcast_to(total, out_ref.shape)
    for j in range(len(far)):
        far_copy(j, z).wait_send()


def total_of(parts, dims):
    ny, nz, nx, ng = dims
    plane = ny * nx * ng
    vm = pl.BlockSpec(memory_space=pltpu.VMEM)
    return pl.pallas_call(
        functools.partial(reduce_kernel, dims),
        in_specs=[vm],
        out_specs=vm,
        out_shape=jax.ShapeDtypeStruct((1, 128), F32),
        scratch_shapes=[pltpu.VMEM((plane, 1, 128), F32), pltpu.VMEM((nz, 1, 128), F32), pltpu.VMEM((1, 1, 128), F32),
                        pltpu.SemaphoreType.DMA((plane,)), pltpu.SemaphoreType.DMA((plane,)),
                        pltpu.SemaphoreType.DMA((nz,)), pltpu.SemaphoreType.DMA((nz,))],
        compiler_params=pltpu.CompilerParams(collective_id=0, has_side_effects=True),
        name="total",
    )(parts)


def shards(dims, echoes, frame_count, clutter_rank, noise_rank, start_basis):
    n, frames, width = echoes.shape
    half = width // 2
    devices = dims[0] * dims[1] * dims[2] * dims[3]
    spot = np.arange(width, dtype=np.float64)
    window = jnp.asarray((np.sin(np.pi * (spot + 0.5) / width) ** 2).astype(np.float32)[None])

    def slot_of(b):
        return (lax.axis_index("space") * dims[3] + lax.axis_index("grp")) * n + b

    far = lambda a: pltpu.with_memory_space_constraint(a, pltpu.HBM)
    st, s, border, masked = subspace(far(echoes), far(frame_count), far(clutter_rank), far(noise_rank),
                                     far(start_basis.T), slot_of)
    back = [(d + 1, d) for d in range(devices - 1)]
    border = lax.ppermute(border, ("space", "grp"), back)
    volume, strength, last = project(masked, frames, st, s, clutter_rank, noise_rank, window, slot_of)
    volume, strength, parts = finish(border, last, window, strength, volume, n)
    total = total_of(parts, dims)[0, 0]
    power = strength.reshape(-1) / (total / (devices * n * half) + 1e-6)
    return volume, power


def solution(mesh):
    dims = (4, 8, 4, mesh.shape["grp"])
    both = ("space", "grp")
    return jax.shard_map(
        functools.partial(shards, dims), mesh=mesh,
        in_specs=(P(both, None, None), P(), P(), P(), P()),
        out_specs=(P(None, both), P(both)), check_vma=False)
```

```python
import functools
import numpy as np
import jax, jax.numpy as jnp
from jax import lax
from jax.experimental import pallas as pl
from jax.experimental.pallas import tpu as pltpu
from jax.sharding import PartitionSpec as P

F32, BF = jnp.float32, jnp.bfloat16
ITERS = 4
CHUNK = 512
EARLY = 0

NT = (((1,), (1,)), ((), ()))
NN = (((1,), (0,)), ((), ()))

def mm(a, b, dims):
    return lax.dot_general(a, b, dims, preferred_element_type=F32)

def split(a):
    hi = a.astype(BF)
    return hi, (a - hi.astype(F32)).astype(BF)

def split3(a):
    hi = a.astype(BF)
    rest = a - hi.astype(F32)
    mid = rest.astype(BF)
    return hi, mid, (rest - mid.astype(F32)).astype(BF)

def spread(tile, row):
    return jnp.take_along_axis(tile, jnp.full((8, 128), row, jnp.int32), axis=0)


GAP = 64


def eliminate(m_ref, s_ref, pairs, k, between):
    tiles = k // 8
    sub = lax.broadcasted_iota(jnp.int32, (8, 128), 0)
    place = lax.broadcasted_iota(jnp.int32, (8, 128), 1)
    lane = place & (GAP - 1)
    tile = {(b, t): m_ref[b, 8 * t:8 * t + 8, :] for b in pairs for t in range(tiles)}
    for p in range(tiles):
        j0 = 8 * p
        inside = (lane >= j0) & (lane < j0 + 8)
        eye = jnp.where(lane == j0 + sub, 1.0, 0.0)
        between(p)
        cols, diag, inverses, pivots, ahead = {}, {}, {}, {}, {}
        for b in pairs:
            diag[b] = jnp.where(inside, eye, tile[b, p])
        for q in range(8):
            pick = place - lane + (j0 + q)
            for b in pairs:
                for t in range(p, tiles):
                    cols[b, q, t] = jnp.take_along_axis(tile[b, t], pick, axis=1)
        for q in range(8):
            for b in pairs:
                pivot = spread(cols[b, 0, p], 0) if q == 0 else ahead[b]
                inv = 1.0 / pivot
                pivots[b] = pivot if q == 0 else jnp.where(sub == q, pivot, pivots[b])
                inverses[b] = inv if q == 0 else jnp.where(sub == q, inv, inverses[b])
                if q < 7:
                    nxt = cols[b, q + 1, p]
                    cross = spread(cols[b, q, p], q + 1) * spread(nxt, q)
                    ahead[b] = spread(nxt, q + 1) - cross * inv
                    f = jnp.where(sub > q, cols[b, q, p], 0.0) * inv
                    for q2 in range(q + 1, 8):
                        cols[b, q2, p] = cols[b, q2, p] - f * spread(cols[b, q2, p], q)
                    diag[b] = diag[b] - f * spread(diag[b], q)
        for b in pairs:
            m_ref[b, j0:j0 + 8, :] = diag[b]
            s_ref[b, j0:j0 + 8, :] = lax.rsqrt(pivots[b])
        if p == tiles - 1:
            break
        for b in pairs:
            solved = diag[b] * inverses[b]
            rest = {t: jnp.where(inside, 0.0, tile[b, t]) for t in range(p + 1, tiles)}
            for q in range(7, -1, -1):
                row = spread(solved, q)
                if q:
                    solved = solved - jnp.where(sub < q, cols[b, q, p] * inverses[b], 0.0) * row
                for t in rest:
                    rest[t] = rest[t] - cols[b, q, t] * row
            for t in rest:
                tile[b, t] = rest[t]


def mm3(a, b, dims=NN):
    (ah, al), (bh, bl) = a, b
    m = ah.shape[0]
    first = mm(jnp.concatenate([ah, al], axis=0), bh, dims)
    return first[:m] + (first[m:] + mm(ah, bl, dims))


def mm6(a, b, dims=NN):
    (ah, am, al), (bh, bm, bl) = a, b
    m = ah.shape[0]
    pair = jnp.concatenate([bh, bm], axis=0 if dims is NT else 1)
    first = mm(jnp.concatenate([ah, am, al], axis=0), pair, dims)
    high, mid = first[:, :128], first[:, 128:]
    return high[:m] + (high[m:2 * m] + mid[:m]) + (mid[m:2 * m] + high[2 * m:] + mm(ah, bl, dims))


def both(parts, h):
    return tuple(jnp.concatenate([a[:h], a[GAP:GAP + h]], axis=0) for a in parts)


def chosen(rows, h):
    lane = lax.broadcasted_iota(jnp.int32, (h, 128), 1)
    return jnp.where(lane < GAP, rows[:h], rows[h:])


def stacked(x, pad):
    lane = lax.broadcasted_iota(jnp.int32, x.shape, 1)
    first, second = jnp.where(lane < GAP, x, 0.0), jnp.where(lane < GAP, 0.0, x)
    if not pad:
        return jnp.concatenate([first, second], axis=0)
    zero = jnp.zeros((pad, 128), F32)
    return jnp.concatenate([first, zero, second, zero], axis=0)


def subspace_kernel(n, count_of, echo_ref, *refs):
    (fc_ref, cr_ref, nr_ref, start_ref, st_ref, s_out_ref, border_ref, x_ref, gh_ref, gl_ref, p_ref, y_ref, a_ref, s_ref) = refs
    step = pl.program_id(0)
    k, frames = start_ref.shape
    lp = gh_ref.shape[2]

    @pl.when(step == 0)
    def _():
        top = frames // 16 * 16
        gh_ref[:, top:, :] = jnp.zeros((n, lp - top, lp), BF)
        gl_ref[:, top:, :] = jnp.zeros((n, lp - top, lp), BF)

    total = fc_ref[count_of(step)]
    row = lax.broadcasted_iota(jnp.int32, (frames, 1), 0)
    top = frames // 16 * 16
    x_ref[step, top:, :] = jnp.zeros((lp - top, x_ref.shape[2]), BF)
    x_ref[step, :frames, :] = jnp.where(row < total, echo_ref[0], jnp.zeros((), BF))
    x = x_ref[step]
    rows, cut = -(-frames // 16) * 16, frames // 256 * 256
    left = mm(x[:rows], x[:cut], NT)
    right = mm(x[cut:rows], x[cut:lp], NT)
    low = jnp.concatenate([left[cut:], jnp.zeros((lp - rows, cut), F32)], axis=0)
    g = jnp.concatenate([left, jnp.concatenate([low.T, right], axis=0)], axis=1)


    gr = lax.broadcasted_iota(jnp.int32, g.shape, 0)
    gc = lax.broadcasted_iota(jnp.int32, g.shape, 1)
    g = g + jnp.where((gr == gc) & (gr >= total) & (gr < frames), 1.0, 0.0)
    hi, lo = split(g)
    gh_ref[step, :g.shape[0], :] = hi
    gl_ref[step, :g.shape[0], :] = lo

    @pl.when(step == n - 1)
    def _():
        blocks = range(n)
        half = k // 2
        pairs = [(b, min(b + 1, n - 1)) for b in range(0, n, 2)]
        spots = [[(i, e * GAP) for i, pair in enumerate(pairs) for e in (0, 1) if pair[e] == b] for b in range(n)]

        def place(ref, b, value):
            for i, at in spots[b]:
                ref[i, 0, at:at + half, :] = value[:half]
                ref[i, 1, at:at + half, :] = value[half:]

        y_ref[0, 0, :, :] = jnp.zeros((128, lp), F32)
        y_ref[0, 0, :k, :frames] = start_ref[...]
        start = split(y_ref[0, 0, :k, :])
        y_ref[...] = jnp.zeros_like(y_ref)
        p_ref[...] = jnp.zeros_like(p_ref)
        for b in range(n):
            place(p_ref, b, mm3(start, (gh_ref[b], gl_ref[b])))

        def forward(b):
            i, at = spots[b][0]
            p = jnp.concatenate([p_ref[i, 0, at:at + half, :], p_ref[i, 1, at:at + half, :]], axis=0)
            place(y_ref, b, mm3(split(p), (gh_ref[b], gl_ref[b])))

        count = range(len(pairs))

        def leaf(mats, between):
            for i in count:
                a_ref[i, :, :] = mats[i]
            eliminate(a_ref, s_ref, count, half, between)
            out = []
            for i in count:
                lower = a_ref[i]
                ri = lax.broadcasted_iota(jnp.int32, lower.shape, 0)
                ci = lax.broadcasted_iota(jnp.int32, lower.shape, 1) & (GAP - 1)
                out.append(jnp.where(ci < ri, lower, jnp.where(ci == ri, 1.0, 0.0)) * s_ref[i])
            return out

        def inverse(moves):
            z = [[split3(p_ref[i, 0]), split3(p_ref[i, 1])] for i in count]
            c11 = [chosen(mm6(both(z[i][0], half), z[i][0], NT), half) for i in count]
            c12, c22 = {}, {}

            def others(i):
                rows = tuple(jnp.concatenate(parts, axis=0) for parts in zip(both(z[i][0], half), both(z[i][1], half)))
                c = mm6(rows, z[i][1], NT)
                c12[i], c22[i] = chosen(c[:k], half), chosen(c[k:], half)

            panels = half // 8
            first = [functools.partial(others, i) for i in count] + moves[:EARLY]

            def run(some, last):
                plan = {}
                for e, m in enumerate(some):
                    plan.setdefault(e * last // max(len(some), 1), []).append(m)
                return lambda p: [m() for m in plan.get(p, [])]

            w11 = leaf(c11, run(first, panels - 1))
            fill = jnp.zeros((128 - half, 128), F32)
            u, ut = [], []
            for i in count:
                x = mm6(split3(w11[i]), split3(stacked(c12[i], GAP - half)))
                x = jnp.concatenate([x, fill], axis=0)
                u.append(x)
                ut.append(both(split3(x.T), half))
            w22 = leaf([c22[i] - chosen(mm6(ut[i], split3(u[i])), half) for i in count],
                       run(moves[EARLY:], panels - 1))
            out = []
            for i in count:
                t = chosen(mm3(ut[i][:2], split(jnp.concatenate([w11[i], fill], axis=0))), half)
                w21 = -mm3(split(w22[i]), split(stacked(t, GAP - half)))
                top = jnp.concatenate([stacked(w11[i], 0), jnp.zeros((k, 128), F32)], axis=1)
                low = jnp.concatenate([stacked(w21, 0), stacked(w22[i], 0)], axis=1)
                out.append(split(jnp.concatenate([top, low], axis=0)))
            return out

        def apply(factors, ref, i):
            rows = mm3(factors, split(jnp.concatenate([ref[i, 0], ref[i, 1]], axis=0)))
            return rows[:k], rows[k:]

        def body(i, carry):
            factors = inverse([functools.partial(forward, b) for b in range(n)])
            for i in count:
                top, low = apply(factors[i], y_ref, i)
                for e in (0, 1):
                    p_ref[i, 0, e * GAP:e * GAP + half, :] = top[e * half:(e + 1) * half]
                    p_ref[i, 1, e * GAP:e * GAP + half, :] = low[e * half:(e + 1) * half]
            return carry

        lax.fori_loop(0, ITERS - 1, body, 0)
        factors = inverse([])
        fill = jnp.zeros((128 - k, lp), F32)
        for i in count:
            top, low = apply(factors[i], p_ref, i)
            for e in (0, 1):
                b = pairs[i][e]
                if spots[b][0] == (i, e * GAP):
                    rows = slice(e * half, (e + 1) * half)
                    st = jnp.concatenate([top[rows], low[rows], fill], axis=0)
                    st_ref[b, :, :] = st.astype(BF)
                    s_out_ref[b, :, :] = st.T.astype(BF)
        slot = count_of(0)
        band = band_of(k, cr_ref[slot], nr_ref[slot])
        basis = st_ref[0, :k, :]
        border_ref[:, :lp] = basis
        border_ref[:, lp:] = (mm(basis, x_ref[0, :, :x_ref.shape[2] // 2], NN) * band).astype(BF)


def subspace(echoes, fc, cr, nr, start, count_of):
    n, frames, width = echoes.shape
    k = start.shape[0]
    lp = -(-frames // 128) * 128
    half_n = -(-n // 2)
    smem = pl.BlockSpec(memory_space=pltpu.SMEM)
    edge = (k, lp + width // 2)
    return pl.pallas_call(
        functools.partial(subspace_kernel, n, count_of),
        grid=(n,),
        in_specs=[pl.BlockSpec((1, frames, width), lambda i: (i, 0, 0)),
                  smem, smem, smem,
                  pl.BlockSpec((k, frames), lambda i: (0, 0))],
        out_specs=[pl.BlockSpec((n, 128, lp), lambda i: (0, 0, 0)),
                   pl.BlockSpec((n, lp, 128), lambda i: (0, 0, 0)),
                   pl.BlockSpec(edge, lambda i: (0, 0)),
                   pl.BlockSpec((n, lp, width), lambda i: (0, 0, 0))],
        out_shape=[jax.ShapeDtypeStruct((n, 128, lp), BF), jax.ShapeDtypeStruct((n, lp, 128), BF),
                   jax.ShapeDtypeStruct(edge, BF), jax.ShapeDtypeStruct((n, lp, width), BF)],
        scratch_shapes=[pltpu.VMEM((n, lp, lp), BF), pltpu.VMEM((n, lp, lp), BF),
                        pltpu.VMEM((half_n, 2, 128, lp), F32), pltpu.VMEM((half_n, 2, 128, lp), F32),
                        pltpu.VMEM((half_n, k // 2, 128), F32), pltpu.VMEM((half_n, k // 2, 128), F32)],
        compiler_params=pltpu.CompilerParams(vmem_limit_bytes=32 << 20),
        name="subspace",
    )(echoes, fc, cr, nr, start)


def project_kernel(n, frames, count_of, x_ref, st_ref, s_ref, cr_ref, nr_ref, win_ref, vol_ref, str_ref, last_ref,
                   coef_ref, prev_ref):
    step = pl.program_id(0)
    width = x_ref.shape[2]
    half = width // 2
    k = coef_ref.shape[0] - 32
    rows = prev_ref.shape[0]

    @pl.when(step == 0)
    def _():
        coef_ref[...] = jnp.zeros_like(coef_ref)
        prev_ref[...] = jnp.zeros_like(prev_ref)

    slot = count_of(step)
    band = band_of(k, cr_ref[slot], nr_ref[slot])
    st, s = st_ref[0, :k, :], s_ref[0, :rows, :]
    for c in range(width // CHUNK):
        at = slice(c * CHUNK, (c + 1) * CHUNK)
        coef_ref[:k, at] = (mm(st, x_ref[0, :, at], NN) * band).astype(BF)

    for c in range(half // CHUNK):
        at, up = slice(c * CHUNK, (c + 1) * CHUNK), slice(half + c * CHUNK, half + (c + 1) * CHUNK)
        low = mm(s, coef_ref[:, at], NN).astype(BF).astype(F32)
        high = mm(s, coef_ref[:, up], NN).astype(BF).astype(F32)
        vol = (prev_ref[:, at] + low * win_ref[:, at])[:frames]
        vol_ref[:, at] = vol
        str_ref[:, at] = jnp.sum(vol * vol, axis=0, keepdims=True) / frames
        prev_ref[:, at] = high * win_ref[:, up]

    @pl.when(step == n - 1)
    def _():
        last_ref[...] = prev_ref[...]


def band_of(k, low, high):
    col = lax.broadcasted_iota(jnp.int32, (k, 1), 0)
    return jnp.where((col >= low) & (col < high), 1.0, 0.0)


def project(masked, frames, st, s, cr, nr, window, count_of):
    n, _, width = masked.shape
    half, lp, k = width // 2, st.shape[2], st.shape[1] - 32
    rows = -(-frames // 16) * 16
    smem = pl.BlockSpec(memory_space=pltpu.SMEM)
    after = lambda i: (0, jnp.maximum(i - 1, 0))
    return pl.pallas_call(
        functools.partial(project_kernel, n, frames, count_of),
        grid=(n,),
        in_specs=[pl.BlockSpec((1, lp, width), lambda i: (i, 0, 0)),
                  pl.BlockSpec((1, 128, lp), lambda i: (i, 0, 0)),
                  pl.BlockSpec((1, lp, 128), lambda i: (i, 0, 0)),
                  smem, smem,
                  pl.BlockSpec((1, width), lambda i: (0, 0))],
        out_specs=[pl.BlockSpec((frames, half), after), pl.BlockSpec((1, half), after),
                   pl.BlockSpec((rows, half), lambda i: (0, 0))],
        out_shape=[jax.ShapeDtypeStruct((frames, n * half), F32), jax.ShapeDtypeStruct((1, n * half), F32),
                   jax.ShapeDtypeStruct((rows, half), F32)],
        scratch_shapes=[pltpu.VMEM((k + 32, width), BF), pltpu.VMEM((rows, half), F32)],
        compiler_params=pltpu.CompilerParams(vmem_limit_bytes=32 << 20),
        cost_estimate=pl.CostEstimate(flops=int(8e9), bytes_accessed=int(12e6), transcendentals=0),
        name="project",
    )(masked, st, s, cr, nr, window)


def border_kernel(n, border_ref, last_ref, win_ref, str_in_ref, vol_in_ref, vol_ref, str_ref, sum_ref, fac_ref):
    frames, half = vol_ref.shape
    rows = last_ref.shape[0]
    k = border_ref.shape[0]
    lp = border_ref.shape[1] - half
    fac_ref[k:, :] = jnp.zeros((128 - k, fac_ref.shape[1]), BF)
    fac_ref[:k, :] = border_ref[...]
    s = fac_ref[:, :lp].astype(F32).T.astype(BF)[:rows]
    done = (n - 1) * half
    parts = jnp.zeros((1, 128), F32)
    for c in range(done // 128):
        at = slice(c * 128, c * 128 + 128)
        parts = parts + str_in_ref[:, at]
    str_ref[:, :done] = str_in_ref[:, :done]
    for c in range(half // CHUNK):
        at = slice(c * CHUNK, (c + 1) * CHUNK)
        low = mm(s, fac_ref[:, lp + c * CHUNK:lp + (c + 1) * CHUNK], NN).astype(BF).astype(F32)
        vol = (last_ref[:, at] + low * win_ref[:, at])[:frames]
        vol_ref[:, at] = vol
        part = jnp.sum(vol * vol, axis=0, keepdims=True) / frames
        str_ref[:, done + c * CHUNK:done + (c + 1) * CHUNK] = part
        for d in range(CHUNK // 128):
            parts = parts + part[:, d * 128:d * 128 + 128]
    sum_ref[0] = parts


def finish(border, last, window, strength, volume, n):
    rows, half = last.shape
    frames = volume.shape[0]
    vm = pl.BlockSpec(memory_space=pltpu.VMEM)
    whole = lambda a: pl.BlockSpec(a.shape, lambda i: (0, 0))
    return pl.pallas_call(
        functools.partial(border_kernel, n),
        grid=(1,),
        in_specs=[whole(border), whole(last), whole(window), whole(strength), pl.BlockSpec(memory_space=pl.ANY)],
        out_specs=[pl.BlockSpec((frames, half), lambda i: (0, n - 1)), whole(strength),
                   pl.BlockSpec((1, 1, 128), lambda i: (0, 0, 0))],
        out_shape=[jax.ShapeDtypeStruct(volume.shape, F32), jax.ShapeDtypeStruct(strength.shape, F32),
                   jax.ShapeDtypeStruct((1, 1, 128), F32)],
        scratch_shapes=[pltpu.VMEM((128, border.shape[1]), BF)],
        input_output_aliases={4: 0},
        compiler_params=pltpu.CompilerParams(vmem_limit_bytes=32 << 20),
        name="finish",
    )(border, last, window, strength, volume)


def reduce_kernel(dims, in_ref, out_ref, near_ref, far_ref, mid_ref, send1, recv1, send2, recv2):
    ny, nz, nx, ng = dims
    plane = ny * nx * ng
    place, core = lax.axis_index("space"), lax.axis_index("grp")
    y, z, x = place // (nz * nx), (place // nx) % nz, place % nx
    me = (y * nx + x) * ng + core

    hop = lambda step, size: min(step, size - step)
    steps = sorted(((dy, dx, dg) for dy in range(ny) for dx in range(nx) for dg in range(ng)),
                   key=lambda d: -hop(d[0], ny) - hop(d[1], nx))
    steps = [d for d in steps if d != (0, 0, 0)]
    ys = [(y + d) % ny for d in range(ny)]
    xs = [(x + d) % nx for d in range(nx)]
    gs = [(core + d) % ng for d in range(ng)]
    zs = [(z + d) % nz for d in range(nz)]
    near = [((ys[dy] * nz + z) * nx + xs[dx], gs[dg]) for dy, dx, dg in steps]
    slots = [(ys[dy] * nx + xs[dx]) * ng + gs[dg] for dy, dx, dg in steps]
    reach = sorted(range(1, nz), key=lambda d: -hop(d, nz))
    far = [((y * nz + zs[d]) * nx + x, core) for d in reach]

    barrier = pltpu.get_barrier_semaphore()
    for peer in far + near:
        pl.semaphore_signal(barrier, inc=1, device_id=peer, device_id_type=pl.DeviceIdType.MESH)
    near_ref[me] = in_ref[0]
    pl.semaphore_wait(barrier, len(near) + len(far))

    def near_copy(j, slot):
        return pltpu.make_async_remote_copy(
            src_ref=in_ref.at[0], dst_ref=near_ref.at[slot], send_sem=send1.at[j], recv_sem=recv1.at[slot],
            device_id=near[j], device_id_type=pl.DeviceIdType.MESH)

    def far_copy(j, slot):
        return pltpu.make_async_remote_copy(
            src_ref=mid_ref.at[0], dst_ref=far_ref.at[slot], send_sem=send2.at[j], recv_sem=recv2.at[slot],
            device_id=far[j], device_id_type=pl.DeviceIdType.MESH)

    for j in range(len(near)):
        near_copy(j, me).start()
    for j in range(len(near)):
        near_copy(j, slots[j]).wait_recv()
    part = jnp.sum(near_ref[...], axis=0)
    mid_ref[0] = part
    far_ref[z] = part
    for j in range(len(far)):
        far_copy(j, z).start()
    for j in range(len(near)):
        near_copy(j, me).wait_send()
    for j in range(len(far)):
        far_copy(j, zs[reach[j]]).wait_recv()
    total = jnp.sum(jnp.sum(far_ref[...], axis=0), axis=1, keepdims=True)
    out_ref[...] = jnp.broadcast_to(total, out_ref.shape)
    for j in range(len(far)):
        far_copy(j, z).wait_send()


def total_of(parts, dims):
    ny, nz, nx, ng = dims
    plane = ny * nx * ng
    vm = pl.BlockSpec(memory_space=pltpu.VMEM)
    return pl.pallas_call(
        functools.partial(reduce_kernel, dims),
        in_specs=[vm],
        out_specs=vm,
        out_shape=jax.ShapeDtypeStruct((1, 128), F32),
        scratch_shapes=[pltpu.VMEM((plane, 1, 128), F32), pltpu.VMEM((nz, 1, 128), F32), pltpu.VMEM((1, 1, 128), F32),
                        pltpu.SemaphoreType.DMA((plane,)), pltpu.SemaphoreType.DMA((plane,)),
                        pltpu.SemaphoreType.DMA((nz,)), pltpu.SemaphoreType.DMA((nz,))],
        compiler_params=pltpu.CompilerParams(collective_id=0, has_side_effects=True),
        name="total",
    )(parts)


def shards(dims, echoes, frame_count, clutter_rank, noise_rank, start_basis):
    n, frames, width = echoes.shape
    half = width // 2
    devices = dims[0] * dims[1] * dims[2] * dims[3]
    spot = np.arange(width, dtype=np.float64)
    window = jnp.asarray((np.sin(np.pi * (spot + 0.5) / width) ** 2).astype(np.float32)[None])

    def slot_of(b):
        return (lax.axis_index("space") * dims[3] + lax.axis_index("grp")) * n + b

    far = lambda a: pltpu.with_memory_space_constraint(a, pltpu.HBM)
    st, s, border, masked = subspace(far(echoes), far(frame_count), far(clutter_rank), far(noise_rank),
                                     far(start_basis.T), slot_of)
    back = [(d + 1, d) for d in range(devices - 1)]
    border = lax.ppermute(border, ("space", "grp"), back)
    volume, strength, last = project(masked, frames, st, s, clutter_rank, noise_rank, window, slot_of)
    volume, strength, parts = finish(border, last, window, strength, volume, n)
    total = total_of(parts, dims)[0, 0]
    power = strength.reshape(-1) / (total / (devices * n * half) + 1e-6)
    return volume, power


def solution(mesh):
    dims = (4, 8, 4, mesh.shape["grp"])
    both = ("space", "grp")
    return jax.shard_map(
        functools.partial(shards, dims), mesh=mesh,
        in_specs=(P(both, None, None), P(), P(), P(), P()),
        out_specs=(P(None, both), P(both)), check_vma=False)
```

```python
import functools
import numpy as np
import jax, jax.numpy as jnp
from jax import lax
from jax.experimental import pallas as pl
from jax.experimental.pallas import tpu as pltpu
from jax.sharding import PartitionSpec as P

F32, BF = jnp.float32, jnp.bfloat16
ITERS = 4
CHUNK = 512
EARLY = 0

NT = (((1,), (1,)), ((), ()))
NN = (((1,), (0,)), ((), ()))

def mm(a, b, dims):
    return lax.dot_general(a, b, dims, preferred_element_type=F32)

def split(a):
    hi = a.astype(BF)
    return hi, (a - hi.astype(F32)).astype(BF)

def split3(a):
    hi = a.astype(BF)
    rest = a - hi.astype(F32)
    mid = rest.astype(BF)
    return hi, mid, (rest - mid.astype(F32)).astype(BF)

def spread(tile, row):
    return jnp.take_along_axis(tile, jnp.full((8, 128), row, jnp.int32), axis=0)


GAP = 64


def eliminate(m_ref, s_ref, pairs, k, between):
    tiles = k // 8
    sub = lax.broadcasted_iota(jnp.int32, (8, 128), 0)
    place = lax.broadcasted_iota(jnp.int32, (8, 128), 1)
    lane = place & (GAP - 1)
    tile = {(b, t): m_ref[b, 8 * t:8 * t + 8, :] for b in pairs for t in range(tiles)}
    for p in range(tiles):
        j0 = 8 * p
        inside = (lane >= j0) & (lane < j0 + 8)
        eye = jnp.where(lane == j0 + sub, 1.0, 0.0)
        between(p)
        cols, diag, inverses, pivots, ahead = {}, {}, {}, {}, {}
        for b in pairs:
            diag[b] = jnp.where(inside, eye, tile[b, p])
        for q in range(8):
            pick = place - lane + (j0 + q)
            for b in pairs:
                for t in range(p, tiles):
                    cols[b, q, t] = jnp.take_along_axis(tile[b, t], pick, axis=1)
        for q in range(8):
            for b in pairs:
                pivot = spread(cols[b, 0, p], 0) if q == 0 else ahead[b]
                inv = 1.0 / pivot
                pivots[b] = pivot if q == 0 else jnp.where(sub == q, pivot, pivots[b])
                inverses[b] = inv if q == 0 else jnp.where(sub == q, inv, inverses[b])
                if q < 7:
                    nxt = cols[b, q + 1, p]
                    cross = spread(cols[b, q, p], q + 1) * spread(nxt, q)
                    ahead[b] = spread(nxt, q + 1) - cross * inv
                    f = jnp.where(sub > q, cols[b, q, p], 0.0) * inv
                    for q2 in range(q + 1, 8):
                        cols[b, q2, p] = cols[b, q2, p] - f * spread(cols[b, q2, p], q)
                    diag[b] = diag[b] - f * spread(diag[b], q)
        for b in pairs:
            m_ref[b, j0:j0 + 8, :] = diag[b]
            s_ref[b, j0:j0 + 8, :] = lax.rsqrt(pivots[b])
        if p == tiles - 1:
            break
        for b in pairs:
            solved = diag[b] * inverses[b]
            rest = {t: jnp.where(inside, 0.0, tile[b, t]) for t in range(p + 1, tiles)}
            for q in range(7, -1, -1):
                row = spread(solved, q)
                if q:
                    solved = solved - jnp.where(sub < q, cols[b, q, p] * inverses[b], 0.0) * row
                for t in rest:
                    rest[t] = rest[t] - cols[b, q, t] * row
            for t in rest:
                tile[b, t] = rest[t]


def mm3(a, b, dims=NN):
    (ah, al), (bh, bl) = a, b
    m = ah.shape[0]
    first = mm(jnp.concatenate([ah, al], axis=0), bh, dims)
    return first[:m] + (first[m:] + mm(ah, bl, dims))


def mm6(a, b, dims=NN):
    (ah, am, al), (bh, bm, bl) = a, b
    m = ah.shape[0]
    pair = jnp.concatenate([bh, bm], axis=0 if dims is NT else 1)
    first = mm(jnp.concatenate([ah, am, al], axis=0), pair, dims)
    high, mid = first[:, :128], first[:, 128:]
    return high[:m] + (high[m:2 * m] + mid[:m]) + (mid[m:2 * m] + high[2 * m:] + mm(ah, bl, dims))


def both(parts, h):
    return tuple(jnp.concatenate([a[:h], a[GAP:GAP + h]], axis=0) for a in parts)


def chosen(rows, h):
    lane = lax.broadcasted_iota(jnp.int32, (h, 128), 1)
    return jnp.where(lane < GAP, rows[:h], rows[h:])


def stacked(x, pad):
    lane = lax.broadcasted_iota(jnp.int32, x.shape, 1)
    first, second = jnp.where(lane < GAP, x, 0.0), jnp.where(lane < GAP, 0.0, x)
    if not pad:
        return jnp.concatenate([first, second], axis=0)
    zero = jnp.zeros((pad, 128), F32)
    return jnp.concatenate([first, zero, second, zero], axis=0)


def subspace_kernel(n, count_of, echo_ref, *refs):
    (fc_ref, cr_ref, nr_ref, start_ref, st_ref, s_out_ref, border_ref, x_ref, gh_ref, gl_ref, p_ref, y_ref, a_ref, s_ref) = refs
    step = pl.program_id(0)
    k, frames = start_ref.shape
    lp = gh_ref.shape[2]

    @pl.when(step == 0)
    def _():
        top = frames // 16 * 16
        gh_ref[:, top:, :] = jnp.zeros((n, lp - top, lp), BF)
        gl_ref[:, top:, :] = jnp.zeros((n, lp - top, lp), BF)

    total = fc_ref[count_of(step)]
    row = lax.broadcasted_iota(jnp.int32, (frames, 1), 0)
    top = frames // 16 * 16
    x_ref[step, top:, :] = jnp.zeros((lp - top, x_ref.shape[2]), BF)
    x_ref[step, :frames, :] = jnp.where(row < total, echo_ref[0], jnp.zeros((), BF))
    x = x_ref[step]
    rows, cut = -(-frames // 16) * 16, frames // 256 * 256
    left = mm(x[:rows], x[:cut], NT)
    right = mm(x[cut:rows], x[cut:lp], NT)
    low = jnp.concatenate([left[cut:], jnp.zeros((lp - rows, cut), F32)], axis=0)
    g = jnp.concatenate([left, jnp.concatenate([low.T, right], axis=0)], axis=1)


    gr = lax.broadcasted_iota(jnp.int32, g.shape, 0)
    gc = lax.broadcasted_iota(jnp.int32, g.shape, 1)
    g = g + jnp.where((gr == gc) & (gr >= total) & (gr < frames), 1.0, 0.0)
    hi, lo = split(g)
    gh_ref[step, :g.shape[0], :] = hi
    gl_ref[step, :g.shape[0], :] = lo

    @pl.when(step == n - 1)
    def _():
        blocks = range(n)
        half = k // 2
        pairs = [(b, min(b + 1, n - 1)) for b in range(0, n, 2)]
        spots = [[(i, e * GAP) for i, pair in enumerate(pairs) for e in (0, 1) if pair[e] == b] for b in range(n)]

        def place(ref, b, value):
            for i, at in spots[b]:
                ref[i, 0, at:at + half, :] = value[:half]
                ref[i, 1, at:at + half, :] = value[half:]

        y_ref[0, 0, :, :] = jnp.zeros((128, lp), F32)
        y_ref[0, 0, :k, :frames] = start_ref[...]
        start = split(y_ref[0, 0, :k, :])
        y_ref[...] = jnp.zeros_like(y_ref)
        p_ref[...] = jnp.zeros_like(p_ref)
        for b in range(n):
            place(p_ref, b, mm3(start, (gh_ref[b], gl_ref[b])))

        def forward(b):
            i, at = spots[b][0]
            p = jnp.concatenate([p_ref[i, 0, at:at + half, :], p_ref[i, 1, at:at + half, :]], axis=0)
            place(y_ref, b, mm3(split(p), (gh_ref[b], gl_ref[b])))

        count = range(len(pairs))

        def leaf(mats, between):
            for i in count:
                a_ref[i, :, :] = mats[i]
            eliminate(a_ref, s_ref, count, half, between)
            out = []
            for i in count:
                lower = a_ref[i]
                ri = lax.broadcasted_iota(jnp.int32, lower.shape, 0)
                ci = lax.broadcasted_iota(jnp.int32, lower.shape, 1) & (GAP - 1)
                out.append(jnp.where(ci < ri, lower, jnp.where(ci == ri, 1.0, 0.0)) * s_ref[i])
            return out

        def inverse(moves):
            z = [[split3(p_ref[i, 0]), split3(p_ref[i, 1])] for i in count]
            c11 = [chosen(mm6(both(z[i][0], half), z[i][0], NT), half) for i in count]
            c12, c22 = {}, {}

            def others(i):
                rows = tuple(jnp.concatenate(parts, axis=0) for parts in zip(both(z[i][0], half), both(z[i][1], half)))
                c = mm6(rows, z[i][1], NT)
                c12[i], c22[i] = chosen(c[:k], half), chosen(c[k:], half)

            panels = half // 8
            first = [functools.partial(others, i) for i in count] + moves[:EARLY]

            def run(some, last):
                plan = {}
                for e, m in enumerate(some):
                    plan.setdefault(e * last // max(len(some), 1), []).append(m)
                return lambda p: [m() for m in plan.get(p, [])]

            w11 = leaf(c11, run(first, panels - 1))
            fill = jnp.zeros((128 - half, 128), F32)
            u, ut = [], []
            for i in count:
                x = mm6(split3(w11[i]), split3(stacked(c12[i], GAP - half)))
                x = jnp.concatenate([x, fill], axis=0)
                u.append(x)
                ut.append(both(split3(x.T), half))
            w22 = leaf([c22[i] - chosen(mm6(ut[i], split3(u[i])), half) for i in count],
                       run(moves[EARLY:], panels - 1))
            out = []
            for i in count:
                t = chosen(mm3(ut[i][:2], split(jnp.concatenate([w11[i], fill], axis=0))), half)
                w21 = -mm3(split(w22[i]), split(stacked(t, GAP - half)))
                top = jnp.concatenate([stacked(w11[i], 0), jnp.zeros((k, 128), F32)], axis=1)
                low = jnp.concatenate([stacked(w21, 0), stacked(w22[i], 0)], axis=1)
                out.append(split(jnp.concatenate([top, low], axis=0)))
            return out

        def apply(factors, ref, i):
            rows = mm3(factors, split(jnp.concatenate([ref[i, 0], ref[i, 1]], axis=0)))
            return rows[:k], rows[k:]

        def body(i, carry):
            factors = inverse([functools.partial(forward, b) for b in range(n)])
            for i in count:
                top, low = apply(factors[i], y_ref, i)
                for e in (0, 1):
                    p_ref[i, 0, e * GAP:e * GAP + half, :] = top[e * half:(e + 1) * half]
                    p_ref[i, 1, e * GAP:e * GAP + half, :] = low[e * half:(e + 1) * half]
            return carry

        lax.fori_loop(0, ITERS - 1, body, 0)
        factors = inverse([])
        fill = jnp.zeros((128 - k, lp), F32)
        for i in count:
            top, low = apply(factors[i], p_ref, i)
            for e in (0, 1):
                b = pairs[i][e]
                if spots[b][0] == (i, e * GAP):
                    rows = slice(e * half, (e + 1) * half)
                    st = jnp.concatenate([top[rows], low[rows], fill], axis=0)
                    st_ref[b, :, :] = st.astype(BF)
                    s_out_ref[b, :, :] = st.T.astype(BF)
        slot = count_of(0)
        band = band_of(k, cr_ref[slot], nr_ref[slot])
        basis = st_ref[0, :k, :]
        border_ref[:, :lp] = basis
        border_ref[:, lp:] = (mm(basis, x_ref[0, :, :x_ref.shape[2] // 2], NN) * band).astype(BF)


def subspace(echoes, fc, cr, nr, start, count_of):
    n, frames, width = echoes.shape
    k = start.shape[0]
    lp = -(-frames // 128) * 128
    half_n = -(-n // 2)
    smem = pl.BlockSpec(memory_space=pltpu.SMEM)
    edge = (k, lp + width // 2)
    return pl.pallas_call(
        functools.partial(subspace_kernel, n, count_of),
        grid=(n,),
        in_specs=[pl.BlockSpec((1, frames, width), lambda i: (i, 0, 0)),
                  smem, smem, smem,
                  pl.BlockSpec((k, frames), lambda i: (0, 0))],
        out_specs=[pl.BlockSpec((n, 128, lp), lambda i: (0, 0, 0)),
                   pl.BlockSpec((n, lp, 128), lambda i: (0, 0, 0)),
                   pl.BlockSpec(edge, lambda i: (0, 0)),
                   pl.BlockSpec((n, lp, width), lambda i: (0, 0, 0))],
        out_shape=[jax.ShapeDtypeStruct((n, 128, lp), BF), jax.ShapeDtypeStruct((n, lp, 128), BF),
                   jax.ShapeDtypeStruct(edge, BF), jax.ShapeDtypeStruct((n, lp, width), BF)],
        scratch_shapes=[pltpu.VMEM((n, lp, lp), BF), pltpu.VMEM((n, lp, lp), BF),
                        pltpu.VMEM((half_n, 2, 128, lp), F32), pltpu.VMEM((half_n, 2, 128, lp), F32),
                        pltpu.VMEM((half_n, k // 2, 128), F32), pltpu.VMEM((half_n, k // 2, 128), F32)],
        compiler_params=pltpu.CompilerParams(vmem_limit_bytes=32 << 20),
        name="subspace",
    )(echoes, fc, cr, nr, start)


def project_kernel(n, frames, count_of, x_ref, st_ref, s_ref, cr_ref, nr_ref, win_ref, vol_ref, str_ref, last_ref,
                   coef_ref, prev_ref):
    step = pl.program_id(0)
    width = x_ref.shape[2]
    half = width // 2
    k = coef_ref.shape[0] - 32
    rows = prev_ref.shape[0]

    @pl.when(step == 0)
    def _():
        coef_ref[...] = jnp.zeros_like(coef_ref)
        prev_ref[...] = jnp.zeros_like(prev_ref)

    slot = count_of(step)
    band = band_of(k, cr_ref[slot], nr_ref[slot])
    st, s = st_ref[0, :k, :], s_ref[0, :rows, :]
    for c in range(width // CHUNK):
        at = slice(c * CHUNK, (c + 1) * CHUNK)
        coef_ref[:k, at] = (mm(st, x_ref[0, :, at], NN) * band).astype(BF)

    for c in range(half // CHUNK):
        at, up = slice(c * CHUNK, (c + 1) * CHUNK), slice(half + c * CHUNK, half + (c + 1) * CHUNK)
        low = mm(s, coef_ref[:, at], NN).astype(BF).astype(F32)
        high = mm(s, coef_ref[:, up], NN).astype(BF).astype(F32)
        vol = (prev_ref[:, at] + low * win_ref[:, at])[:frames]
        vol_ref[:, at] = vol
        str_ref[:, at] = jnp.sum(vol * vol, axis=0, keepdims=True) / frames
        prev_ref[:, at] = high * win_ref[:, up]

    @pl.when(step == n - 1)
    def _():
        last_ref[...] = prev_ref[...]


def band_of(k, low, high):
    col = lax.broadcasted_iota(jnp.int32, (k, 1), 0)
    return jnp.where((col >= low) & (col < high), 1.0, 0.0)


def project(masked, frames, st, s, cr, nr, window, count_of):
    n, _, width = masked.shape
    half, lp, k = width // 2, st.shape[2], st.shape[1] - 32
    rows = -(-frames // 16) * 16
    smem = pl.BlockSpec(memory_space=pltpu.SMEM)
    after = lambda i: (0, jnp.maximum(i - 1, 0))
    return pl.pallas_call(
        functools.partial(project_kernel, n, frames, count_of),
        grid=(n,),
        in_specs=[pl.BlockSpec((1, lp, width), lambda i: (i, 0, 0)),
                  pl.BlockSpec((1, 128, lp), lambda i: (i, 0, 0)),
                  pl.BlockSpec((1, lp, 128), lambda i: (i, 0, 0)),
                  smem, smem,
                  pl.BlockSpec((1, width), lambda i: (0, 0))],
        out_specs=[pl.BlockSpec((frames, half), after), pl.BlockSpec((1, half), after),
                   pl.BlockSpec((rows, half), lambda i: (0, 0))],
        out_shape=[jax.ShapeDtypeStruct((frames, n * half), F32), jax.ShapeDtypeStruct((1, n * half), F32),
                   jax.ShapeDtypeStruct((rows, half), F32)],
        scratch_shapes=[pltpu.VMEM((k + 32, width), BF), pltpu.VMEM((rows, half), F32)],
        compiler_params=pltpu.CompilerParams(vmem_limit_bytes=32 << 20),
        cost_estimate=pl.CostEstimate(flops=int(8e9), bytes_accessed=int(12e6), transcendentals=0),
        name="project",
    )(masked, st, s, cr, nr, window)


def border_kernel(n, border_ref, last_ref, win_ref, str_in_ref, vol_in_ref, vol_ref, str_ref, sum_ref, fac_ref):
    frames, half = vol_ref.shape
    rows = last_ref.shape[0]
    k = border_ref.shape[0]
    lp = border_ref.shape[1] - half
    fac_ref[k:, :] = jnp.zeros((128 - k, fac_ref.shape[1]), BF)
    fac_ref[:k, :] = border_ref[...]
    s = fac_ref[:, :lp].astype(F32).T.astype(BF)[:rows]
    done = (n - 1) * half
    parts = jnp.zeros((1, 128), F32)
    for c in range(done // 128):
        at = slice(c * 128, c * 128 + 128)
        parts = parts + str_in_ref[:, at]
    str_ref[:, :done] = str_in_ref[:, :done]
    for c in range(half // CHUNK):
        at = slice(c * CHUNK, (c + 1) * CHUNK)
        low = mm(s, fac_ref[:, lp + c * CHUNK:lp + (c + 1) * CHUNK], NN).astype(BF).astype(F32)
        vol = (last_ref[:, at] + low * win_ref[:, at])[:frames]
        vol_ref[:, at] = vol
        part = jnp.sum(vol * vol, axis=0, keepdims=True) / frames
        str_ref[:, done + c * CHUNK:done + (c + 1) * CHUNK] = part
        for d in range(CHUNK // 128):
            parts = parts + part[:, d * 128:d * 128 + 128]
    sum_ref[0] = parts


def finish(border, last, window, strength, volume, n):
    rows, half = last.shape
    frames = volume.shape[0]
    vm = pl.BlockSpec(memory_space=pltpu.VMEM)
    whole = lambda a: pl.BlockSpec(a.shape, lambda i: (0, 0))
    return pl.pallas_call(
        functools.partial(border_kernel, n),
        grid=(1,),
        in_specs=[whole(border), whole(last), whole(window), whole(strength), pl.BlockSpec(memory_space=pl.ANY)],
        out_specs=[pl.BlockSpec((frames, half), lambda i: (0, n - 1)), whole(strength),
                   pl.BlockSpec((1, 1, 128), lambda i: (0, 0, 0))],
        out_shape=[jax.ShapeDtypeStruct(volume.shape, F32), jax.ShapeDtypeStruct(strength.shape, F32),
                   jax.ShapeDtypeStruct((1, 1, 128), F32)],
        scratch_shapes=[pltpu.VMEM((128, border.shape[1]), BF)],
        input_output_aliases={4: 0},
        compiler_params=pltpu.CompilerParams(vmem_limit_bytes=32 << 20),
        name="finish",
    )(border, last, window, strength, volume)


def reduce_kernel(dims, in_ref, out_ref, near_ref, far_ref, mid_ref, send1, recv1, send2, recv2):
    ny, nz, nx, ng = dims
    plane = ny * nx * ng
    place, core = lax.axis_index("space"), lax.axis_index("grp")
    y, z, x = place // (nz * nx), (place // nx) % nz, place % nx
    me = (y * nx + x) * ng + core

    hop = lambda step, size: min(step, size - step)
    steps = sorted(((dy, dx, dg) for dy in range(ny) for dx in range(nx) for dg in range(ng)),
                   key=lambda d: -hop(d[0], ny) - hop(d[1], nx))
    steps = [d for d in steps if d != (0, 0, 0)]
    ys = [(y + d) % ny for d in range(ny)]
    xs = [(x + d) % nx for d in range(nx)]
    gs = [(core + d) % ng for d in range(ng)]
    zs = [(z + d) % nz for d in range(nz)]
    near = [((ys[dy] * nz + z) * nx + xs[dx], gs[dg]) for dy, dx, dg in steps]
    slots = [(ys[dy] * nx + xs[dx]) * ng + gs[dg] for dy, dx, dg in steps]
    reach = sorted(range(1, nz), key=lambda d: -hop(d, nz))
    far = [((y * nz + zs[d]) * nx + x, core) for d in reach]

    barrier = pltpu.get_barrier_semaphore()
    for peer in far + near:
        pl.semaphore_signal(barrier, inc=1, device_id=peer, device_id_type=pl.DeviceIdType.MESH)
    near_ref[me] = in_ref[0]
    pl.semaphore_wait(barrier, len(near) + len(far))

    def near_copy(j, slot):
        return pltpu.make_async_remote_copy(
            src_ref=in_ref.at[0], dst_ref=near_ref.at[slot], send_sem=send1.at[j], recv_sem=recv1.at[slot],
            device_id=near[j], device_id_type=pl.DeviceIdType.MESH)

    def far_copy(j, slot):
        return pltpu.make_async_remote_copy(
            src_ref=mid_ref.at[0], dst_ref=far_ref.at[slot], send_sem=send2.at[j], recv_sem=recv2.at[slot],
            device_id=far[j], device_id_type=pl.DeviceIdType.MESH)

    for j in range(len(near)):
        near_copy(j, me).start()
    for j in range(len(near)):
        near_copy(j, slots[j]).wait_recv()
    part = jnp.sum(near_ref[...], axis=0)
    mid_ref[0] = part
    far_ref[z] = part
    for j in range(len(far)):
        far_copy(j, z).start()
    for j in range(len(near)):
        near_copy(j, me).wait_send()
    for j in range(len(far)):
        far_copy(j, zs[reach[j]]).wait_recv()
    total = jnp.sum(jnp.sum(far_ref[...], axis=0), axis=1, keepdims=True)
    out_ref[...] = jnp.broadcast_to(total, out_ref.shape)
    for j in range(len(far)):
        far_copy(j, z).wait_send()


def total_of(parts, dims):
    ny, nz, nx, ng = dims
    plane = ny * nx * ng
    vm = pl.BlockSpec(memory_space=pltpu.VMEM)
    return pl.pallas_call(
        functools.partial(reduce_kernel, dims),
        in_specs=[vm],
        out_specs=vm,
        out_shape=jax.ShapeDtypeStruct((1, 128), F32),
        scratch_shapes=[pltpu.VMEM((plane, 1, 128), F32), pltpu.VMEM((nz, 1, 128), F32), pltpu.VMEM((1, 1, 128), F32),
                        pltpu.SemaphoreType.DMA((plane,)), pltpu.SemaphoreType.DMA((plane,)),
                        pltpu.SemaphoreType.DMA((nz,)), pltpu.SemaphoreType.DMA((nz,))],
        compiler_params=pltpu.CompilerParams(collective_id=0, has_side_effects=True, vmem_limit_bytes=8 << 20),
        name="total",
    )(parts)


def shards(dims, echoes, frame_count, clutter_rank, noise_rank, start_basis):
    n, frames, width = echoes.shape
    half = width // 2
    devices = dims[0] * dims[1] * dims[2] * dims[3]
    spot = np.arange(width, dtype=np.float64)
    window = jnp.asarray((np.sin(np.pi * (spot + 0.5) / width) ** 2).astype(np.float32)[None])

    def slot_of(b):
        return (lax.axis_index("space") * dims[3] + lax.axis_index("grp")) * n + b

    far = lambda a: pltpu.with_memory_space_constraint(a, pltpu.HBM)
    st, s, border, masked = subspace(far(echoes), far(frame_count), far(clutter_rank), far(noise_rank),
                                     far(start_basis.T), slot_of)
    back = [(d + 1, d) for d in range(devices - 1)]
    border = lax.ppermute(border, ("space", "grp"), back)
    volume, strength, last = project(masked, frames, st, s, clutter_rank, noise_rank, window, slot_of)
    volume, strength, parts = finish(border, last, window, strength, volume, n)
    total = total_of(parts, dims)[0, 0]
    power = strength.reshape(-1) / (total / (devices * n * half) + 1e-6)
    return volume, power


def solution(mesh):
    dims = (4, 8, 4, mesh.shape["grp"])
    both = ("space", "grp")
    return jax.shard_map(
        functools.partial(shards, dims), mesh=mesh,
        in_specs=(P(both, None, None), P(), P(), P(), P()),
        out_specs=(P(None, both), P(both)), check_vma=False)
```
